256 devices in a mesh: row: 32 (over z, x_hi, core), col: 8 (over y, x_lo).
Axes of the slice: x: 4 (x_hi: 2, x_lo: 2; x = x_hi * 2 + x_lo), y: 4, z: 8, core: 2. Of those that a mesh axis runs over, the one named last changes fastest.
Arguments:
- qkv: bfloat16 [512, 64, 3, 3072], P('row', 'col'), may hold values from -6 to 6
- cotangent: bfloat16 [512, 64, 3072], P('row', 'col'), may hold values from -6 to 6
- norm_gains: float32 [2, 128], replicated, may hold values from 0.1 to 1.9
- rel_table: float32 [24, 15, 15], replicated, may hold values from -6 to 250
- shifts: int32 [2], replicated, may hold values from 1 to 7
- mask_ids: int32 [512, 64], replicated, may hold values from 0 to 2
Outputs:
- attention: bfloat16 [512, 64, 3072], P('row', 'col')
- d_qkv: bfloat16 [512, 64, 3, 3072], P('row', 'col')
- d_gains: float32 [2, 128], replicated
- d_table: float32 [24, 15, 15], replicated
The draws below stay inside these ranges and needn't reach their ends.
All inputs are finite; a program needn't handle non-finite values.
Results may differ from the reference program's by a relative error of at most 0.0073.
Values may be sent and summed in bfloat16 or wider, within the bound.
No kernel may reach another device: no remote copies, remote signals or barrier semaphores. Data moves between devices by JAX's collectives and lax.ppermute only.
A program may use at most 192 MiB of HBM per device.

```python
import math
import jax
import jax.numpy as jnp
from jax import lax

WIN = 8
NH = 24
HD = 128
FEATURES = 3072
SPAN = 15
ROWS = 512
COLS = 64


def draw_rel_table(key, part):
    base = jnp.clip(jax.random.normal(jax.random.fold_in(key, 11), (NH, SPAN, SPAN), jnp.float32), -6.0, 6.0)
    return base


def with_ends(array, own_key, low, top_value):
    spot = [jax.random.randint(jax.random.fold_in(own_key, axis), (), 0, length) for axis, length in enumerate(array.shape)]
    main_axis = array.shape.index(max(array.shape))
    next_to = spot[:main_axis] + [(spot[main_axis] + 1) % array.shape[main_axis]] + spot[main_axis + 1:]
    return array.at[tuple(spot)].set(low).at[tuple(next_to)].set(top_value)


def shard_levels(own_key, extent, shards, least, largest):
    def one(position, shards_of):
        steps = jax.random.uniform(jax.random.fold_in(jax.random.fold_in(own_key, 6), position), (shards_of,), jnp.float32, least / len(shards), largest / len(shards))
        return jnp.repeat(jnp.exp(steps), extent[position] // shards_of).reshape((-1,) + (1,) * (len(extent) - position - 1))

    gain = one(*shards[0])
    for cut in shards[1:]:
        gain = gain * one(*cut)
    return gain


def bell_draw(own_key, dims, scale, most, split=(), kind=jnp.bfloat16):
    array = scale * jax.random.normal(own_key, dims, jnp.float32)
    if split:
        array = array * shard_levels(own_key, dims, split, -0.22, 0.18)
    return jnp.clip(array, -most, most).astype(kind)


def setup_inputs(seed: int = 0) -> dict:
    seeds = jax.random.split(jax.random.key(seed), 7)
    qkv = bell_draw(seeds[0], (ROWS, COLS, 3, FEATURES), 1.0, 6.0, ((0, 32), (1, 8)))
    cotangent = bell_draw(seeds[1], (ROWS, COLS, FEATURES), 1.0, 6.0, ((0, 32), (1, 8)))
    norm_gains = jnp.clip(1.0 + 0.18 * jax.random.normal(seeds[2], (2, HD), jnp.float32), 0.1, 1.9)
    rel_table = draw_rel_table(jax.random.fold_in(seeds[6], 71), 0)
    shifts = jax.random.randint(seeds[4], (2,), 1, WIN).astype(jnp.int32)
    mask_ids = with_ends(jax.random.randint(seeds[5], (ROWS, COLS), 0, 3), jax.random.fold_in(seeds[5], 1), 0, 2).astype(jnp.int32)
    return {"qkv": qkv, "cotangent": cotangent, "norm_gains": norm_gains, "rel_table": rel_table, "shifts": shifts, "mask_ids": mask_ids}


EPSILON = 1e-06
NEG_FILL = -1e+30

def head_norm(inputs, gain_vec):
    values = inputs.astype(jnp.float32)
    average = lax.optimization_barrier(jnp.mean(values, axis=-1, keepdims=True))
    centred = values - average
    variance = lax.optimization_barrier(jnp.mean(centred * centred, axis=-1, keepdims=True))
    inv_sigma = lax.rsqrt(variance + EPSILON)
    x_hat = centred * inv_sigma
    return (x_hat, inv_sigma, (x_hat * gain_vec).astype(jnp.bfloat16))

def norm_back(x_hat, inv_sigma, d_normed, gain_vec):
    d_hat = d_normed * gain_vec
    first_mean = lax.optimization_barrier(jnp.mean(d_hat, axis=-1, keepdims=True))
    second_mean = lax.optimization_barrier(jnp.mean(d_hat * x_hat, axis=-1, keepdims=True))
    d_input = inv_sigma * (d_hat - first_mean - x_hat * second_mean)
    d_gain = lax.optimization_barrier(jnp.sum(d_normed * x_hat, axis=tuple(range(d_normed.ndim - 1))))
    return (d_input, d_gain)

def offset_table(window_size):
    span_count = 2 * window_size - 1
    places = jnp.arange(window_size * window_size, dtype=jnp.int32)
    row_pos = places // window_size
    col_pos = places % window_size
    code_grid = (row_pos[:, None] - row_pos[None, :] + window_size - 1) * span_count + (col_pos[:, None] - col_pos[None, :] + window_size - 1)
    codes = jnp.arange(span_count * span_count, dtype=jnp.int32)
    return (code_grid[:, :, None] == codes[None, None, :]).astype(jnp.float32)

def to_windows(field, window_size):
    row_count, col_count = (field.shape[0], field.shape[1])
    trailing = field.shape[2:]
    blocks = field.reshape((row_count // window_size, window_size, col_count // window_size, window_size) + trailing)
    blocks = jnp.moveaxis(blocks, 2, 1)
    return blocks.reshape((row_count // window_size * (col_count // window_size), window_size * window_size) + trailing)

def from_windows(blocks, window_size, row_count, col_count):
    trailing = blocks.shape[2:]
    field = blocks.reshape((row_count // window_size, col_count // window_size, window_size, window_size) + trailing)
    field = jnp.moveaxis(field, 1, 2)
    return field.reshape((row_count, col_count) + trailing)

def product(form, left, right):
    return jnp.einsum(form, left.astype(jnp.float32), right.astype(jnp.float32))

def window_core(q_norm, k_norm, values, grads, pos_bias, allowed, score_scale):
    scores = product('wqhd,wkhd->whqk', q_norm, k_norm) * score_scale + pos_bias[None]
    scores = jnp.where(allowed[:, None], scores, NEG_FILL)
    row_max = lax.optimization_barrier(jnp.max(scores, axis=-1, keepdims=True))
    weights = jnp.exp(scores - row_max)
    probs = weights / lax.optimization_barrier(jnp.sum(weights, axis=-1, keepdims=True))
    probs_b = probs.astype(jnp.bfloat16)
    output = product('whqk,wkhd->wqhd', probs_b, values)
    d_probs = product('wqhd,wkhd->whqk', grads, values)
    row_dot = lax.optimization_barrier(jnp.sum(probs * d_probs, axis=-1, keepdims=True))
    d_scores = probs * (d_probs - row_dot)
    d_scores_b = d_scores.astype(jnp.bfloat16)
    d_qnorm = product('whqk,wkhd->wqhd', d_scores_b, k_norm) * score_scale
    d_knorm = product('whqk,wqhd->wkhd', d_scores_b, q_norm) * score_scale
    d_value = product('whqk,wqhd->wkhd', probs_b, grads)
    return (output, d_qnorm, d_knorm, d_value, lax.optimization_barrier(jnp.sum(d_scores, axis=0)))

def reference(qkv, cotangent, norm_gains, rel_table, shifts, mask_ids):
    shift_row = shifts[0]
    shift_col = shifts[1]
    score_scale = 1.0 / math.sqrt(HD)
    one_hot = offset_table(WIN)
    pos_bias = jnp.einsum('hc,qkc->hqk', rel_table.reshape(NH, SPAN * SPAN), one_hot, precision=lax.Precision.HIGHEST)
    labels = jnp.roll(mask_ids, (-shift_row, -shift_col), (0, 1))

    def one_band(band_index):
        row_index = ((band_index * WIN + shift_row + jnp.arange(WIN, dtype=jnp.int32)) % ROWS).astype(jnp.int32)
        band_qkv = jnp.roll(jnp.take(qkv, row_index, axis=0), -shift_col, axis=1)
        band_grad = jnp.roll(jnp.take(cotangent, row_index, axis=0), -shift_col, axis=1)
        band_labels = lax.dynamic_slice_in_dim(labels, (band_index * WIN).astype(jnp.int32), WIN, 0)
        fields = band_qkv.reshape(WIN, COLS, 3, NH, HD)
        q_hat, q_inv, q_norm = head_norm(fields[:, :, 0], norm_gains[0])
        k_hat, k_inv, k_norm = head_norm(fields[:, :, 1], norm_gains[1])
        label_win = to_windows(band_labels, WIN)
        allowed = label_win[:, :, None] == label_win[:, None, :]
        output, d_qnorm, d_knorm, d_value, d_bias = window_core(to_windows(q_norm, WIN), to_windows(k_norm, WIN), to_windows(fields[:, :, 2], WIN), to_windows(band_grad.reshape(WIN, COLS, NH, HD), WIN), pos_bias, allowed, score_scale)
        output = from_windows(output, WIN, WIN, COLS)
        d_qnorm = from_windows(d_qnorm, WIN, WIN, COLS)
        d_knorm = from_windows(d_knorm, WIN, WIN, COLS)
        d_value = from_windows(d_value, WIN, WIN, COLS)
        d_query, dgain_q = norm_back(q_hat, q_inv, d_qnorm, norm_gains[0])
        d_key, dgain_k = norm_back(k_hat, k_inv, d_knorm, norm_gains[1])
        packed = jnp.stack([output, d_query, d_key, d_value], axis=2).reshape(WIN, COLS, 4, NH * HD).astype(jnp.bfloat16)
        return (packed, d_bias, jnp.stack([dgain_q, dgain_k]))
    packed, d_bias, d_gain = lax.map(one_band, jnp.arange(ROWS // WIN, dtype=jnp.int32))
    packed = jnp.roll(packed.reshape(ROWS, COLS, 4, NH * HD), (shift_row, shift_col), (0, 1))
    d_table = jnp.einsum('hqk,qkc->hc', lax.optimization_barrier(jnp.sum(d_bias, axis=0)), one_hot, precision=lax.Precision.HIGHEST)
    return (packed[:, :, 0], packed[:, :, 1:], lax.optimization_barrier(jnp.sum(d_gain, axis=0)), d_table.reshape(NH, SPAN, SPAN))
```

```python
import functools
import math

import jax
import jax.numpy as jnp
from jax import lax
from jax.experimental import pallas as pl
from jax.experimental.pallas import tpu as pltpu
from jax.sharding import Mesh
from jax.sharding import PartitionSpec as P

ROW = ("row_0", "row_1", "row_2")
COL = ("col_0", "col_1")
ROW_COL = ("row_0", "row_1", "row_2", "col_0", "col_1")

EPSILON = 1e-06
NEG_FILL = -1e30
WIN = 8
HALF = 4
HD = 128
STEP_HEADS = 4


def shifted(value, axis, steps):
    count = lax.axis_size(axis)
    pairs = [(source, (source + steps) % count) for source in range(count)]
    return lax.ppermute(value, axis, pairs)


def pulled(slot, shift, extent):
    low = jnp.where(shift <= HALF, 0, shift + extent - WIN)
    return (slot >= low) & (slot < jnp.where(shift <= HALF, shift, extent))


def head_norm(values, gain_vec):
    centred = values - jnp.mean(values, axis=-1, keepdims=True)
    variance = jnp.mean(centred * centred, axis=-1, keepdims=True)
    inv_sigma = lax.rsqrt(variance + EPSILON)
    x_hat = centred * inv_sigma
    return x_hat, inv_sigma, (x_hat * gain_vec).astype(jnp.bfloat16)


def norm_back(x_hat, inv_sigma, d_hat):
    first_mean = jnp.mean(d_hat, axis=-1, keepdims=True)
    second_mean = jnp.mean(d_hat * x_hat, axis=-1, keepdims=True)
    return inv_sigma * (d_hat - first_mean - x_hat * second_mean)


def fold_rows(values):
    return functools.reduce(jnp.add, [values[i * 8 : i * 8 + 8] for i in range(values.shape[0] // 8)])


def matmul(left, right, left_dim, right_dim, **kwargs):
    return lax.dot_general(
        left, right, (((left_dim,), (right_dim,)), ((), ())), preferred_element_type=jnp.float32, **kwargs
    )


def window_kernel(
    spec, qkv, cot, hcol, hrow, table, gains, labels, att, dqkv, sums, x_all, mask, table_grad, gain_grad
):
    step = pl.program_id(0)
    steps = pl.num_programs(0)
    shift_row, shift_col, grid_row, grid_col = spec[0], spec[1], spec[2], spec[3]
    tokens = 128
    col_place = lambda col: (col - shift_col) & 7
    score_scale = 1.0 / math.sqrt(HD)

    @pl.when(step == 0)
    def _():
        cols = labels.shape[0]
        rows = labels.shape[1]
        col_turn = jnp.where(shift_col <= HALF, WIN, cols - WIN)
        row_turn = jnp.where(shift_row <= HALF, 16, rows - 16)
        lane = lax.broadcasted_iota(jnp.int32, (8, 128), 1)
        sub = lax.broadcasted_iota(jnp.int32, (8, 128), 0)

        def labels_at(first_row):
            base = pl.multiple_of((first_row // 128) * 128, 128)
            here = labels[pl.ds(pl.multiple_of(grid_col, 8), 8), pl.ds(base, 128)]
            there = labels[pl.ds(pl.multiple_of((grid_col + col_turn) % cols, 8), 8), pl.ds(base, 128)]
            both = jnp.where(pulled(sub, shift_col, WIN), there, here).astype(jnp.float32)
            return pltpu.roll(both, (128 - first_row % 128) % 128, 1)

        slots = jnp.where(
            pulled(lane, shift_row, 16), labels_at((grid_row + row_turn) % rows), labels_at(grid_row)
        )
        across = jnp.concatenate([jnp.broadcast_to(slots[:, i : i + 1], (8, 128)) for i in range(16)], axis=0)
        query = lax.broadcasted_iota(jnp.int32, (tokens, tokens), 0) // 8
        key = lax.broadcasted_iota(jnp.int32, (tokens, tokens), 1) // 8
        same = (((query - shift_row) & 15) // 8) == (((key - shift_row) & 15) // 8)
        mask[...] = jnp.where(same & (across == across.T), 0.0, NEG_FILL)
        gain_grad[...] = jnp.zeros_like(gain_grad)

    def comp(ref, row, part, lanes):
        return ref[row, part, :, lanes] if ref is not cot else ref[row, :, lanes]

    for head in range(STEP_HEADS):
        lanes = slice(head * HD, head * HD + HD)
        for part in range(4):
            source = qkv if part < 3 else cot
            for row in range(16):
                x_all[head * 4 + part, row * 8 : row * 8 + 8, :] = comp(source, row, part, lanes).astype(jnp.float32)
    for i in range(HALF):
        row = jnp.where(shift_row <= HALF, i, i + 12)

        @pl.when(pulled(row, shift_row, 16))
        def _():
            start = pl.multiple_of(row * 8, 8)
            for head in range(STEP_HEADS):
                lanes = slice(head * HD, head * HD + HD)
                for part in range(4):
                    x_all[head * 4 + part, pl.ds(start, 8), :] = hrow[i, part, :, lanes].astype(jnp.float32)

    for i in range(HALF):
        col = jnp.where(shift_col <= HALF, i, i + HALF)

        @pl.when(pulled(col, shift_col, WIN))
        def _():
            for head in range(STEP_HEADS):
                lanes = slice(head * HD, head * HD + HD)
                for part in range(4):
                    x_all[head * 4 + part, pl.ds(col, 16, stride=8), :] = hcol[i, part, :, lanes].astype(jnp.float32)

    sub = lax.broadcasted_iota(jnp.int32, (8, 128), 0)
    lane = lax.broadcasted_iota(jnp.int32, (8, 128), 1)
    col_code = col_place(sub) - col_place(lane & 7) + WIN - 1
    gain_q = gains[0:1, :]
    gain_k = gains[1:2, :]
    for head in range(STEP_HEADS):
        lanes = slice(head * HD, head * HD + HD)
        q_hat, q_inv, q_norm = head_norm(x_all[head * 4], gain_q)
        k_hat, k_inv, k_norm = head_norm(x_all[head * 4 + 1], gain_k)
        values = x_all[head * 4 + 2].astype(jnp.bfloat16)
        grads = x_all[head * 4 + 3].astype(jnp.bfloat16)
        diagonal = jnp.zeros((8, 128), jnp.float32)
        for y in range(15):
            diagonal = jnp.where(col_code == y, table[head, y : y + 1, :], diagonal)
        bias = jnp.concatenate([pltpu.roll(diagonal, (row * 8 - 56) % 128, 1) for row in range(16)], axis=0)
        scores = matmul(q_norm, k_norm, 1, 1) * score_scale + bias + mask[...]
        weights = jnp.exp(scores - jnp.max(scores, axis=-1, keepdims=True))
        probs = weights * (1.0 / jnp.sum(weights, axis=-1, keepdims=True))
        probs_b = probs.astype(jnp.bfloat16)
        att[:, :, lanes] = matmul(probs_b, values, 1, 0).reshape(16, 8, HD).astype(jnp.bfloat16)
        d_probs = matmul(grads, values, 1, 1)
        row_dot = jnp.sum(probs * d_probs, axis=-1, keepdims=True)
        d_scores = probs * (d_probs - row_dot)
        d_scores_b = d_scores.astype(jnp.bfloat16)
        folded = functools.reduce(
            jnp.add,
            [pltpu.roll(d_scores[row * 8 : row * 8 + 8], (56 - row * 8) % 128, 1) for row in range(16)],
        )
        by_code = [jnp.sum(jnp.where(col_code == y, folded, 0.0), axis=0, keepdims=True) for y in range(15)]
        table_grad[pl.ds(pl.multiple_of((step * STEP_HEADS + head) * 16, 16), 16), :] = jnp.concatenate(
            by_code + [jnp.zeros((1, 128), jnp.float32)], axis=0
        )
        dqkv[:, 2, :, lanes] = matmul(probs_b, grads, 0, 0).reshape(16, 8, HD).astype(jnp.bfloat16)
        d_qnorm = matmul(d_scores_b, k_norm, 1, 0)
        gain_grad[0] += fold_rows(d_qnorm * q_hat)
        d_query = norm_back(q_hat, q_inv, d_qnorm * (gain_q * score_scale))
        dqkv[:, 0, :, lanes] = d_query.reshape(16, 8, HD).astype(jnp.bfloat16)
        d_knorm = matmul(d_scores_b, q_norm, 0, 0)
        gain_grad[1] += fold_rows(d_knorm * k_hat)
        d_key = norm_back(k_hat, k_inv, d_knorm * (gain_k * score_scale))
        dqkv[:, 1, :, lanes] = d_key.reshape(16, 8, HD).astype(jnp.bfloat16)

    @pl.when(step == steps - 1)
    def _():
        group = lax.broadcasted_iota(jnp.int32, (16, 128), 0)
        member = lax.broadcasted_iota(jnp.int32, (16, 128), 1) // 8
        pick = jnp.where((group == member) & (group < 15), 1.0, 0.0)
        by_offset = matmul(pick, table_grad[...], 1, 1, precision=lax.Precision.HIGHEST)
        gain_q_sum = jnp.sum(gain_grad[0], axis=0, keepdims=True) * score_scale
        gain_k_sum = jnp.sum(gain_grad[1], axis=0, keepdims=True) * score_scale
        last = jnp.concatenate([gain_q_sum, gain_k_sum, jnp.zeros_like(gain_k_sum)], axis=1)
        is_last = lax.broadcasted_iota(jnp.int32, by_offset.shape, 0) == 15
        sums[...] = jnp.where(is_last, last, by_offset)


def run_windows(spec, qkv, cot, hcol, hrow, table, gains, labels):
    head_count = table.shape[0]
    width = STEP_HEADS * HD
    return pl.pallas_call(
        window_kernel,
        grid_spec=pltpu.PrefetchScalarGridSpec(
            num_scalar_prefetch=1,
            grid=(head_count // STEP_HEADS,),
            in_specs=[
                pl.BlockSpec((16, 3, 8, width), lambda i, s: (0, 0, 0, i)),
                pl.BlockSpec((16, 8, width), lambda i, s: (0, 0, i)),
                pl.BlockSpec((HALF, 4, 16, width), lambda i, s: (0, 0, 0, i)),
                pl.BlockSpec((HALF, 4, 8, width), lambda i, s: (0, 0, 0, i)),
                pl.BlockSpec((STEP_HEADS, 16, 128), lambda i, s: (i, 0, 0)),
                pl.BlockSpec((2, 128), lambda i, s: (0, 0)),
                pl.BlockSpec(labels.shape, lambda i, s: (0, 0)),
            ],
            out_specs=[
                pl.BlockSpec((16, 8, width), lambda i, s: (0, 0, i)),
                pl.BlockSpec((16, 3, 8, width), lambda i, s: (0, 0, 0, i)),
                pl.BlockSpec((16, head_count * 16), lambda i, s: (0, 0)),
            ],
            scratch_shapes=[
                pltpu.VMEM((STEP_HEADS * 4, 128, HD), jnp.float32),
                pltpu.VMEM((128, 128), jnp.float32),
                pltpu.VMEM((head_count * 16, 128), jnp.float32),
                pltpu.VMEM((2, 8, 128), jnp.float32),
            ],
        ),
        out_shape=[
            jax.ShapeDtypeStruct(cot.shape, jnp.bfloat16),
            jax.ShapeDtypeStruct(qkv.shape, jnp.bfloat16),
            jax.ShapeDtypeStruct((16, head_count * 16), jnp.float32),
        ],
        compiler_params=pltpu.CompilerParams(dimension_semantics=("arbitrary",)),
        name="windows",
    )(spec, qkv, cot, hcol, hrow, table, gains, labels)


def exchange(shift, extent, axis, towards_owner, pieces):
    def branch(s):
        low, high, steps = (0, s, -1) if s <= HALF else (s + extent - WIN, extent, 1)
        if towards_owner:
            steps = -steps

        def run():
            received = shifted(pieces(low, high), axis, steps)
            first = low % HALF
            spare = (first, HALF - first - (high - low), 0)
            return lax.pad(received, jnp.zeros((), received.dtype), (spare,) + ((0, 0, 0),) * (received.ndim - 1))

        return run

    return lax.switch(shift - 1, [branch(s) for s in range(1, WIN)])


def stack_parts(qkv, cot):
    return jnp.concatenate([qkv, cot[:, None]], axis=1)


def fill_rows(own, strip, shift_row):
    slot = lax.broadcasted_iota(jnp.int32, own.shape, 0)
    zeros = jnp.zeros((16 - 2 * HALF,) + own.shape[1:], own.dtype)
    return jnp.where(pulled(slot, shift_row, 16), jnp.concatenate([strip, zeros, strip], axis=0), own)


def fill_cols(own, strip, shift_col):
    slot = lax.broadcasted_iota(jnp.int32, own.shape, 2)
    turned = jnp.transpose(strip, (2, 1, 0, 3))
    return jnp.where(pulled(slot, shift_col, WIN), jnp.concatenate([turned, turned], axis=2), own)


def local(qkv, cotangent, norm_gains, rel_table, shifts, mask_ids):
    head_count = rel_table.shape[0]
    shift_row = shifts[0]
    shift_col = shifts[1]
    spec = jnp.stack([shift_row, shift_col, lax.axis_index(ROW) * 16, lax.axis_index(COL) * 8]).astype(jnp.int32)
    qkv_t = jnp.transpose(qkv, (0, 2, 1, 3))
    by_col = jnp.transpose(jnp.flip(rel_table, 1), (0, 2, 1))
    table = jnp.pad(jnp.repeat(by_col, 8, axis=2), ((0, 0), (0, 1), (0, 8)))

    hrow = exchange(shift_row, 16, ROW, False, lambda a, b: stack_parts(qkv_t[a:b], cotangent[a:b]))
    filled = fill_rows(stack_parts(qkv_t, cotangent), hrow, shift_row)
    hcol = exchange(shift_col, WIN, COL, False, lambda a, b: jnp.transpose(filled[:, :, a:b], (2, 1, 0, 3)))
    att, dqkv, sums = run_windows(spec, qkv_t, cotangent, hcol, hrow, table, norm_gains, mask_ids.T)
    back_row = exchange(shift_row, 16, ROW, True, lambda a, b: stack_parts(dqkv[a:b], att[a:b]))
    filled = fill_rows(stack_parts(dqkv, att), back_row, shift_row)
    back_col = exchange(shift_col, WIN, COL, True, lambda a, b: jnp.transpose(filled[:, :, a:b], (2, 1, 0, 3)))
    merged = fill_cols(filled, back_col, shift_col)
    sums = lax.psum(sums, ROW_COL)
    d_gains = sums[15, : 2 * HD].reshape(2, HD)
    d_table = jnp.transpose(jnp.flip(sums[:15], 0).reshape(15, head_count, 16)[:, :, :15], (1, 0, 2))
    return (merged[:, 3], jnp.transpose(merged[:, :3], (0, 2, 1, 3)), d_gains, d_table)


def solution(mesh):
    torus = Mesh(mesh.devices.reshape(8, 2, 2, 4, 2), ROW_COL)
    placed = (P(ROW, COL, None, None), P(ROW, COL, None), P(), P(), P(), P())
    return jax.shard_map(
        local,
        mesh=torus,
        in_specs=placed,
        out_specs=(P(ROW, COL, None), P(ROW, COL, None, None), P(), P()),
        check_vma=False,
    )
```

```python
import functools
import math

import jax
import jax.numpy as jnp
from jax import lax
from jax.experimental import pallas as pl
from jax.experimental.pallas import tpu as pltpu
from jax.sharding import Mesh
from jax.sharding import PartitionSpec as P

ROW = ("row_0", "row_1", "row_2")
COL = ("col_0", "col_1")
ROW_COL = ("row_0", "row_1", "row_2", "col_0", "col_1")

EPSILON = 1e-06
NEG_FILL = -1e30
WIN = 8
HALF = 4
HD = 128
WINDOW_HEADS = 6
MOVE_HEADS = 12


def shifted(value, axis, steps):
    count = lax.axis_size(axis)
    pairs = [(source, (source + steps) % count) for source in range(count)]
    return lax.ppermute(value, axis, pairs)


def pulled(slot, shift, extent):
    low = jnp.where(shift <= HALF, 0, shift + extent - WIN)
    return (slot >= low) & (slot < jnp.where(shift <= HALF, shift, extent))


def head_norm(values, gain_vec):
    centred = values - jnp.mean(values, axis=-1, keepdims=True)
    variance = jnp.mean(centred * centred, axis=-1, keepdims=True)
    inv_sigma = lax.rsqrt(variance + EPSILON)
    x_hat = centred * inv_sigma
    return x_hat, inv_sigma, (x_hat * gain_vec).astype(jnp.bfloat16)


def norm_back(x_hat, inv_sigma, d_hat):
    first_mean = jnp.mean(d_hat, axis=-1, keepdims=True)
    second_mean = jnp.mean(d_hat * x_hat, axis=-1, keepdims=True)
    return inv_sigma * (d_hat - first_mean - x_hat * second_mean)


def fold_rows(values):
    return functools.reduce(jnp.add, [values[i * 8 : i * 8 + 8] for i in range(values.shape[0] // 8)])


def matmul(left, right, left_dim, right_dim, **kwargs):
    return lax.dot_general(
        left, right, (((left_dim,), (right_dim,)), ((), ())), preferred_element_type=jnp.float32, **kwargs
    )


def split(index, size):
    return index // size, index % size


def iotas(rows, cols):
    return (lax.broadcasted_iota(jnp.int32, (rows, cols), 0), lax.broadcasted_iota(jnp.int32, (rows, cols), 1))


def one_hot(condition):
    return jnp.where(condition, 1.0, 0.0).astype(jnp.bfloat16)


def strip_of_slots(spec, rows, cols):
    place, slot = iotas(rows, cols)
    (col, row), (slot_row, slot_col) = split(place, 16), split(slot, 8)
    return (row == slot_row) & (col + jnp.where(spec[1] <= HALF, 0, HALF) == slot_col)


def slots_of_strip(spec, rows, cols):
    slot, place = iotas(rows, cols)
    (col, row), (slot_row, slot_col) = split(place, 16), split(slot, 8)
    taken = (row == slot_row) & (col + jnp.where(spec[1] <= HALF, 0, HALF) == slot_col)
    return taken & pulled(slot_col, spec[1], WIN)


def row_slot(spec, place):
    row, col = split(place, 8)
    return row + jnp.where(spec[0] <= HALF, 0, 12), col


def tile_of(own_qkv, own_att, part, lanes):
    own = own_qkv[:, part, :, lanes] if part < 3 else own_att[:, :, lanes]
    return own.astype(jnp.float32).reshape(128, HD)


def row_strip_of(rows, part, lanes):
    return rows[:, part, :, lanes].astype(jnp.float32).reshape(32, HD).astype(jnp.bfloat16)


def put_tile(dqkv, att, part, lanes, result):
    rows = result.reshape(16, 8, HD).astype(jnp.bfloat16)
    if part < 3:
        dqkv[:, part, :, lanes] = rows
    else:
        att[:, :, lanes] = rows


def put_strip(strip, part, lanes, result):
    strip[:, part, :, lanes] = result.astype(jnp.bfloat16).reshape(HALF, 16, HD)


def each_part():
    return [(part, slice(head * HD, head * HD + HD)) for head in range(MOVE_HEADS) for part in range(4)]


def pack_kernel(spec, qkv, cot, hrow, strip, own_pick, row_pick):
    @pl.when(pl.program_id(0) == 0)
    def _():
        _, slot = iotas(64, 128)
        own_pick[...] = one_hot(strip_of_slots(spec, 64, 128) & ~pulled(slot // 8, spec[0], 16))
        place, source = iotas(64, 32)
        row, col = row_slot(spec, source)
        place_col, place_row = split(place, 16)
        same = (place_row == row) & (place_col + jnp.where(spec[1] <= HALF, 0, HALF) == col)
        row_pick[...] = one_hot(same & pulled(row, spec[0], 16))

    for part, lanes in each_part():
        own = tile_of(qkv, cot, part, lanes).astype(jnp.bfloat16)
        rows = row_strip_of(hrow, part, lanes)
        put_strip(strip, part, lanes, matmul(own_pick[...], own, 1, 0) + matmul(row_pick[...], rows, 1, 0))


def rows_kernel(spec, own_qkv, own_att, strip, rows, pick):
    @pl.when(pl.program_id(0) == 0)
    def _():
        slot, place = iotas(32, 64)
        row, slot_col = row_slot(spec, slot)
        col, place_row = split(place, 16)
        pick[...] = one_hot((row == place_row) & (col + jnp.where(spec[1] <= HALF, 0, HALF) == slot_col))

    slot, _ = iotas(32, HD)
    taken = pulled(slot % 8, spec[1], WIN)
    for part, lanes in each_part():
        own = own_qkv[:, part, :, lanes] if part < 3 else own_att[:, :, lanes]
        moved = matmul(pick[...], strip[:, part, :, lanes].reshape(64, HD), 1, 0)
        merged = jnp.where(taken, moved, own.astype(jnp.float32).reshape(32, HD))
        rows[:, part, :, lanes] = merged.reshape(HALF, 8, HD).astype(jnp.bfloat16)


def merge_kernel(spec, own_qkv, own_att, strip, rows, dqkv, att, pick):
    @pl.when(pl.program_id(0) == 0)
    def _():
        slot, place = iotas(128, 32)
        row, col = row_slot(spec, place)
        slot_row, slot_col = split(slot, 8)
        by_row = (slot_row == row) & (slot_col == col) & pulled(row, spec[0], 16)
        slot, _ = iotas(128, 64)
        by_col = slots_of_strip(spec, 128, 64) & ~pulled(slot // 8, spec[0], 16)
        pick[...] = jnp.concatenate([one_hot(by_col), one_hot(by_row)], axis=1)

    slot, _ = iotas(128, HD)
    taken = pulled(slot % 8, spec[1], WIN) | pulled(slot // 8, spec[0], 16)
    for part, lanes in each_part():
        back = jnp.concatenate([strip[:, part, :, lanes].reshape(64, HD), row_strip_of(rows, part, lanes)], axis=0)
        moved = matmul(pick[...], back, 1, 0)
        put_tile(dqkv, att, part, lanes, jnp.where(taken, moved, tile_of(own_qkv, own_att, part, lanes)))


def window_kernel(
    spec, qkv, cot, hcol, hrow, table, gains, labels, att, dqkv, strip, sums, mask, table_grad, gain_grad, pick, send_pick
):
    step = pl.program_id(0)
    steps = pl.num_programs(0)
    shift_row, shift_col, grid_row, grid_col = spec[0], spec[1], spec[2], spec[3]
    tokens = 128
    col_place = lambda col: (col - shift_col) & 7
    score_scale = 1.0 / math.sqrt(HD)

    @pl.when(step == 0)
    def _():
        cols = labels.shape[0]
        rows = labels.shape[1]
        col_turn = jnp.where(shift_col <= HALF, WIN, cols - WIN)
        row_turn = jnp.where(shift_row <= HALF, 16, rows - 16)
        lane = lax.broadcasted_iota(jnp.int32, (8, 128), 1)
        sub = lax.broadcasted_iota(jnp.int32, (8, 128), 0)

        def labels_at(first_row):
            base = pl.multiple_of((first_row // 128) * 128, 128)
            here = labels[pl.ds(pl.multiple_of(grid_col, 8), 8), pl.ds(base, 128)]
            there = labels[pl.ds(pl.multiple_of((grid_col + col_turn) % cols, 8), 8), pl.ds(base, 128)]
            both = jnp.where(pulled(sub, shift_col, WIN), there, here).astype(jnp.float32)
            return pltpu.roll(both, (128 - first_row % 128) % 128, 1)

        slots = jnp.where(
            pulled(lane, shift_row, 16), labels_at((grid_row + row_turn) % rows), labels_at(grid_row)
        )
        across = jnp.concatenate([jnp.broadcast_to(slots[:, i : i + 1], (8, 128)) for i in range(16)], axis=0)
        query = lax.broadcasted_iota(jnp.int32, (tokens, tokens), 0) // 8
        key = lax.broadcasted_iota(jnp.int32, (tokens, tokens), 1) // 8
        same = (((query - shift_row) & 15) // 8) == (((key - shift_row) & 15) // 8)
        mask[...] = jnp.where(same & (across == across.T), 0.0, NEG_FILL)
        gain_grad[...] = jnp.zeros_like(gain_grad)
        slot, place = iotas(tokens, 32)
        row, col = row_slot(spec, place)
        slot_row, slot_col = split(slot, 8)
        by_row = (slot_row == row) & (slot_col == col) & pulled(row, shift_row, 16)
        by_row = one_hot(by_row & ~pulled(slot_col, shift_col, WIN))
        pick[...] = jnp.concatenate([one_hot(slots_of_strip(spec, tokens, 64)), by_row], axis=1)
        send_pick[...] = one_hot(strip_of_slots(spec, 64, tokens))

    slot, _ = iotas(tokens, HD)
    taken = pulled(slot % 8, shift_col, WIN) | pulled(slot // 8, shift_row, 16)

    def load(head, part):
        lanes = slice(head * HD, head * HD + HD)
        moved = jnp.concatenate(
            [hcol[:, part, :, lanes].reshape(64, HD), row_strip_of(hrow, part, lanes)], axis=0
        )
        return jnp.where(taken, matmul(pick[...], moved, 1, 0), tile_of(qkv, cot, part, lanes))

    def put(head, part, result):
        lanes = slice(head * HD, head * HD + HD)
        put_tile(dqkv, att, part, lanes, result)
        put_strip(strip, part, lanes, matmul(send_pick[...], result.astype(jnp.bfloat16), 1, 0))

    sub = lax.broadcasted_iota(jnp.int32, (8, 128), 0)
    lane = lax.broadcasted_iota(jnp.int32, (8, 128), 1)
    col_code = col_place(sub) - col_place(lane & 7) + WIN - 1
    gain_q = gains[0:1, :]
    gain_k = gains[1:2, :]

    heads = range(WINDOW_HEADS)

    queries = [head_norm(load(head, 0), gain_q) for head in heads]
    keys = [head_norm(load(head, 1), gain_k) for head in heads]
    values = [load(head, 2).astype(jnp.bfloat16) for head in heads]
    grads = [load(head, 3).astype(jnp.bfloat16) for head in heads]

    def bias(head):
        diagonal = jnp.zeros((8, 128), jnp.float32)
        for y in range(15):
            diagonal = jnp.where(col_code == y, table[head, y : y + 1, :], diagonal)
        return jnp.concatenate([pltpu.roll(diagonal, (row * 8 - 56) % 128, 1) for row in range(16)], axis=0)

    scores = [
        matmul(queries[head][2], keys[head][2], 1, 1) * score_scale + bias(head) + mask[...] for head in heads
    ]
    d_probs = [matmul(grads[head], values[head], 1, 1) for head in heads]
    tops = [jnp.max(scores[head], axis=-1, keepdims=True) for head in heads]
    weights = [jnp.exp(scores[head] - tops[head]) for head in heads]
    inverses = [1.0 / jnp.sum(weights[head], axis=-1, keepdims=True) for head in heads]
    row_dots = [jnp.sum(weights[head] * d_probs[head], axis=-1, keepdims=True) for head in heads]
    probs = [weights[head] * inverses[head] for head in heads]
    d_scores = [probs[head] * (d_probs[head] - row_dots[head] * inverses[head]) for head in heads]
    probs_b = [probs[head].astype(jnp.bfloat16) for head in heads]
    d_scores_b = [d_scores[head].astype(jnp.bfloat16) for head in heads]
    for head in heads:
        put(head, 3, matmul(probs_b[head], values[head], 1, 0))
        put(head, 2, matmul(probs_b[head], grads[head], 0, 0))
    d_qnorms = [matmul(d_scores_b[head], keys[head][2], 1, 0) for head in heads]
    d_knorms = [matmul(d_scores_b[head], queries[head][2], 0, 0) for head in heads]
    for head in heads:
        folded = functools.reduce(
            jnp.add,
            [pltpu.roll(d_scores[head][row * 8 : row * 8 + 8], (56 - row * 8) % 128, 1) for row in range(16)],
        )
        by_code = [jnp.sum(jnp.where(col_code == y, folded, 0.0), axis=0, keepdims=True) for y in range(15)]
        table_grad[pl.ds(pl.multiple_of((step * WINDOW_HEADS + head) * 16, 16), 16), :] = jnp.concatenate(
            by_code + [jnp.zeros((1, 128), jnp.float32)], axis=0
        )
    gain_grad[0] += functools.reduce(jnp.add, [fold_rows(d_qnorms[head] * queries[head][0]) for head in heads])
    gain_grad[1] += functools.reduce(jnp.add, [fold_rows(d_knorms[head] * keys[head][0]) for head in heads])
    for head in heads:
        put(head, 0, norm_back(queries[head][0], queries[head][1], d_qnorms[head] * (gain_q * score_scale)))
        put(head, 1, norm_back(keys[head][0], keys[head][1], d_knorms[head] * (gain_k * score_scale)))

    @pl.when(step == steps - 1)
    def _():
        group = lax.broadcasted_iota(jnp.int32, (16, 128), 0)
        member = lax.broadcasted_iota(jnp.int32, (16, 128), 1) // 8
        pick = jnp.where((group == member) & (group < 15), 1.0, 0.0)
        by_offset = matmul(pick, table_grad[...], 1, 1, precision=lax.Precision.HIGHEST)
        gain_q_sum = jnp.sum(gain_grad[0], axis=0, keepdims=True) * score_scale
        gain_k_sum = jnp.sum(gain_grad[1], axis=0, keepdims=True) * score_scale
        last = jnp.concatenate([gain_q_sum, gain_k_sum, jnp.zeros_like(gain_k_sum)], axis=1)
        is_last = lax.broadcasted_iota(jnp.int32, by_offset.shape, 0) == 15
        sums[...] = jnp.where(is_last, last, by_offset)


def qkv_spec(heads):
    return pl.BlockSpec((16, 3, 8, heads * HD), lambda i, s: (0, 0, 0, i))


def cot_spec(heads):
    return pl.BlockSpec((16, 8, heads * HD), lambda i, s: (0, 0, i))


def strip_spec(heads):
    return pl.BlockSpec((HALF, 4, 16, heads * HD), lambda i, s: (0, 0, 0, i))


def rows_spec(heads):
    return pl.BlockSpec((HALF, 4, 8, heads * HD), lambda i, s: (0, 0, 0, i))


def PICK(rows, cols):
    return pltpu.VMEM((rows, cols), jnp.bfloat16)


def bf16(*dims):
    return jax.ShapeDtypeStruct(dims, jnp.bfloat16)


def call(kernel, grid, in_specs, out_specs, out_shape, scratch, name, **kwargs):
    return pl.pallas_call(
        kernel,
        grid_spec=pltpu.PrefetchScalarGridSpec(
            num_scalar_prefetch=1, grid=grid, in_specs=in_specs, out_specs=out_specs, scratch_shapes=scratch
        ),
        out_shape=out_shape,
        compiler_params=pltpu.CompilerParams(dimension_semantics=("arbitrary",) * len(grid)),
        name=name,
        **kwargs,
    )


def pack_cols(spec, qkv, cot, hrow):
    width = cot.shape[2]
    n = MOVE_HEADS
    return call(
        pack_kernel,
        (width // (n * HD),),
        [qkv_spec(n), cot_spec(n), rows_spec(n)],
        strip_spec(n),
        bf16(HALF, 4, 16, width),
        [PICK(64, 128), PICK(64, 32)],
        "pack",
    )(spec, qkv, cot, hrow)


def pack_rows(spec, dqkv, att, strip):
    width = att.shape[2]
    n = MOVE_HEADS
    block = lambda s: jnp.where(s[0] <= HALF, 0, 3)
    return call(
        rows_kernel,
        (width // (n * HD),),
        [
            pl.BlockSpec((HALF, 3, 8, n * HD), lambda i, s: (block(s), 0, 0, i)),
            pl.BlockSpec((HALF, 8, n * HD), lambda i, s: (block(s), 0, i)),
            strip_spec(n),
        ],
        rows_spec(n),
        bf16(HALF, 4, 8, width),
        [PICK(32, 64)],
        "rows",
    )(spec, dqkv, att, strip)


def merge(spec, dqkv, att, strip, rows):
    width = att.shape[2]
    n = MOVE_HEADS
    return call(
        merge_kernel,
        (width // (n * HD),),
        [qkv_spec(n), cot_spec(n), strip_spec(n), rows_spec(n)],
        [qkv_spec(n), cot_spec(n)],
        [bf16(*dqkv.shape), bf16(*att.shape)],
        [PICK(128, 96)],
        "merge",
        cost_estimate=pl.CostEstimate(flops=2 * 10**9, transcendentals=0, bytes_accessed=9 * 10**6),
    )(spec, dqkv, att, strip, rows)


def run_windows(spec, qkv, cot, hcol, hrow, table, gains, labels):
    head_count = table.shape[0]
    n = WINDOW_HEADS
    return call(
        window_kernel,
        (head_count // n,),
        [
            qkv_spec(n),
            cot_spec(n),
            strip_spec(n),
            rows_spec(n),
            pl.BlockSpec((n, 16, 128), lambda i, s: (i, 0, 0)),
            pl.BlockSpec((2, 128), lambda i, s: (0, 0)),
            pl.BlockSpec(labels.shape, lambda i, s: (0, 0)),
        ],
        [cot_spec(n), qkv_spec(n), strip_spec(n), pl.BlockSpec((16, head_count * 16), lambda i, s: (0, 0))],
        [
            bf16(*cot.shape),
            bf16(*qkv.shape),
            bf16(*hcol.shape),
            jax.ShapeDtypeStruct((16, head_count * 16), jnp.float32),
        ],
        [
            pltpu.VMEM((128, 128), jnp.float32),
            pltpu.VMEM((head_count * 16, 128), jnp.float32),
            pltpu.VMEM((2, 8, 128), jnp.float32),
            PICK(128, 96),
            PICK(64, 128),
        ],
        "windows",
    )(spec, qkv, cot, hcol, hrow, table, gains, labels)


def spread(received, low):
    first = low % HALF
    spare = (first, HALF - first - received.shape[0], 0)
    return lax.pad(received, jnp.zeros((), received.dtype), (spare,) + ((0, 0, 0),) * (received.ndim - 1))


def by_case(shift, branch):
    case = (shift > 2).astype(jnp.int32) + (shift > HALF) + (shift > 5)
    return lax.switch(case, [branch(0, 2, -1), branch(0, 4, -1), branch(1, 4, 1), branch(2, 4, 1)])


def pull_rows(shift, pieces, beside):
    def branch(first, last, steps):
        turn = 0 if steps < 0 else 12
        return lambda: (spread(shifted(pieces(first + turn, last + turn), ROW, steps), first), beside())

    return by_case(shift, branch)


def pull_cols(shift, packed):
    def branch(s):
        first, last, steps = (0, s, -1) if s <= HALF else (s - HALF, HALF, 1)
        return lambda: spread(shifted(packed[first:last], COL, steps), first)

    return lax.switch(shift - 1, [branch(s) for s in range(1, WIN)])


def doubled(sums, rounds):
    for axis, bit in rounds:
        sums = sums + lax.ppermute(sums, axis, [(i, i ^ bit) for i in range(lax.axis_size(axis))])
    return sums


def give_back(shift, axis, strip, sums, rounds):
    def branch(first, last, steps):
        return lambda: (spread(shifted(strip[first:last], axis, -steps), first), doubled(sums, rounds))

    return by_case(shift, branch)


def local(qkv, cotangent, norm_gains, rel_table, shifts, mask_ids):
    head_count = rel_table.shape[0]
    shift_row = shifts[0]
    shift_col = shifts[1]
    qkv_t = jnp.transpose(qkv, (0, 2, 1, 3))

    def row_pieces(low, high):
        return jnp.concatenate([qkv_t[low:high], cotangent[low:high, None]], axis=1)

    def tables():
        places = [lax.axis_index(ROW) * 16, lax.axis_index(COL) * 8]
        by_col = jnp.transpose(jnp.flip(rel_table, 1), (0, 2, 1))
        spread_out = jnp.pad(jnp.repeat(by_col, 8, axis=2), ((0, 0), (0, 1), (0, 8)))
        return jnp.stack([shift_row, shift_col] + places).astype(jnp.int32), spread_out

    hrow, (spec, table) = pull_rows(shift_row, row_pieces, tables)
    packed = pack_cols(spec, qkv_t, cotangent, hrow)
    hcol = pull_cols(shift_col, packed)
    att, dqkv, strip, sums = run_windows(spec, qkv_t, cotangent, hcol, hrow, table, norm_gains, mask_ids.T)
    strip, sums = give_back(shift_col, COL, strip, sums, (("row_0", 1), ("row_0", 2), ("row_0", 4)))
    rows = pack_rows(spec, dqkv, att, strip)
    rows, sums = give_back(shift_row, ROW, rows, sums, (("col_0", 1), ("col_0", 2)))
    dqkv, att = merge(spec, dqkv, att, strip, rows)
    sums = doubled(sums, (("row_2", 1), ("col_1", 1), ("row_1", 1)))
    d_gains = sums[15, : 2 * HD].reshape(2, HD)
    d_table = jnp.transpose(jnp.flip(sums[:15], 0).reshape(15, head_count, 16)[:, :, :15], (1, 0, 2))
    return (att, jnp.transpose(dqkv, (0, 2, 1, 3)), d_gains, d_table)


def solution(mesh):
    torus = Mesh(mesh.devices.reshape(8, 2, 2, 4, 2), ROW_COL)
    placed = (P(ROW, COL, None, None), P(ROW, COL, None), P(), P(), P(), P())
    return jax.shard_map(
        local,
        mesh=torus,
        in_specs=placed,
        out_specs=(P(ROW, COL, None), P(ROW, COL, None, None), P(), P()),
        check_vma=False,
    )
```

```python
import functools
import math

import jax
import jax.numpy as jnp
from jax import lax
from jax.experimental import pallas as pl
from jax.experimental.pallas import tpu as pltpu
from jax.sharding import Mesh
from jax.sharding import PartitionSpec as P

ROW = ("row_0", "row_1", "row_2")
COL = ("col_0", "col_1")
ROW_COL = ("row_0", "row_1", "row_2", "col_0", "col_1")

EPSILON = 1e-06
NEG_FILL = -1e30
WIN = 8
HALF = 4
HD = 128
WINDOW_HEADS = 6
MOVE_HEADS = 12
PAIR = 256


def shifted(value, axis, steps):
    count = lax.axis_size(axis)
    pairs = [(source, (source + steps) % count) for source in range(count)]
    return lax.ppermute(value, axis, pairs)


def pulled(slot, shift, extent):
    low = jnp.where(shift <= HALF, 0, shift + extent - WIN)
    return (slot >= low) & (slot < jnp.where(shift <= HALF, shift, extent))


def head_norm(values, gain_vec):
    centred = values - jnp.mean(values, axis=-1, keepdims=True)
    variance = jnp.mean(centred * centred, axis=-1, keepdims=True)
    inv_sigma = lax.rsqrt(variance + EPSILON)
    x_hat = centred * inv_sigma
    return x_hat, inv_sigma, (x_hat * gain_vec).astype(jnp.bfloat16)


def norm_back(x_hat, inv_sigma, d_hat):
    first_mean = jnp.mean(d_hat, axis=-1, keepdims=True)
    second_mean = jnp.mean(d_hat * x_hat, axis=-1, keepdims=True)
    return inv_sigma * (d_hat - first_mean - x_hat * second_mean)


def fold_rows(values):
    return functools.reduce(jnp.add, [values[i * 8 : i * 8 + 8] for i in range(values.shape[0] // 8)])


def matmul(left, right, left_dim, right_dim, **kwargs):
    return lax.dot_general(
        left, right, (((left_dim,), (right_dim,)), ((), ())), preferred_element_type=jnp.float32, **kwargs
    )


def split(index, size):
    return index // size, index % size


def iotas(rows, cols):
    return (lax.broadcasted_iota(jnp.int32, (rows, cols), 0), lax.broadcasted_iota(jnp.int32, (rows, cols), 1))


def one_hot(condition):
    return jnp.where(condition, 1.0, 0.0).astype(jnp.bfloat16)


def strip_of_slots(spec, rows, cols):
    place, slot = iotas(rows, cols)
    (col, row), (slot_row, slot_col) = split(place, 16), split(slot, 8)
    return (row == slot_row) & (col + jnp.where(spec[1] <= HALF, 0, HALF) == slot_col)


def slots_of_strip(spec, rows, cols):
    slot, place = iotas(rows, cols)
    (col, row), (slot_row, slot_col) = split(place, 16), split(slot, 8)
    taken = (row == slot_row) & (col + jnp.where(spec[1] <= HALF, 0, HALF) == slot_col)
    return taken & pulled(slot_col, spec[1], WIN)


def row_slot(spec, place):
    row, col = split(place, 8)
    return row + jnp.where(spec[0] <= HALF, 0, 12), col


def tile_of(own_qkv, own_att, part, lanes):
    own = own_qkv[:, part, :, lanes] if part < 3 else own_att[:, :, lanes]
    return own.astype(jnp.float32).reshape(128, PAIR)


def row_strip_of(rows, part, lanes):
    return rows[:, part, :, lanes].astype(jnp.float32).reshape(32, PAIR).astype(jnp.bfloat16)


def put_tile(dqkv, att, part, lanes, result):
    rows = result.reshape(16, 8, PAIR).astype(jnp.bfloat16)
    if part < 3:
        dqkv[:, part, :, lanes] = rows
    else:
        att[:, :, lanes] = rows


def put_strip(strip, part, lanes, result):
    strip[:, part, :, lanes] = result.astype(jnp.bfloat16).reshape(HALF, 16, PAIR)


def each_part():
    return [(part, slice(at, at + PAIR)) for at in range(0, MOVE_HEADS * HD, PAIR) for part in range(4)]


def pack_kernel(spec, qkv, cot, hrow, strip, own_pick, row_pick):
    @pl.when(pl.program_id(0) == 0)
    def _():
        _, slot = iotas(64, 128)
        own_pick[...] = one_hot(strip_of_slots(spec, 64, 128) & ~pulled(slot // 8, spec[0], 16))
        place, source = iotas(64, 32)
        row, col = row_slot(spec, source)
        place_col, place_row = split(place, 16)
        same = (place_row == row) & (place_col + jnp.where(spec[1] <= HALF, 0, HALF) == col)
        row_pick[...] = one_hot(same & pulled(row, spec[0], 16))

    for part, lanes in each_part():
        own = tile_of(qkv, cot, part, lanes).astype(jnp.bfloat16)
        rows = row_strip_of(hrow, part, lanes)
        put_strip(strip, part, lanes, matmul(own_pick[...], own, 1, 0) + matmul(row_pick[...], rows, 1, 0))


def rows_kernel(spec, own_qkv, own_att, strip, rows, pick):
    @pl.when(pl.program_id(0) == 0)
    def _():
        slot, place = iotas(32, 64)
        row, slot_col = row_slot(spec, slot)
        col, place_row = split(place, 16)
        pick[...] = one_hot((row == place_row) & (col + jnp.where(spec[1] <= HALF, 0, HALF) == slot_col))

    slot, _ = iotas(32, PAIR)
    taken = pulled(slot % 8, spec[1], WIN)
    for part, lanes in each_part():
        own = own_qkv[:, part, :, lanes] if part < 3 else own_att[:, :, lanes]
        moved = matmul(pick[...], strip[:, part, :, lanes].reshape(64, PAIR), 1, 0)
        merged = jnp.where(taken, moved, own.astype(jnp.float32).reshape(32, PAIR))
        rows[:, part, :, lanes] = merged.reshape(HALF, 8, PAIR).astype(jnp.bfloat16)


def merge_kernel(spec, own_qkv, own_att, strip, rows, dqkv, att, pick):
    @pl.when(pl.program_id(0) == 0)
    def _():
        slot, place = iotas(128, 32)
        row, col = row_slot(spec, place)
        slot_row, slot_col = split(slot, 8)
        by_row = (slot_row == row) & (slot_col == col) & pulled(row, spec[0], 16)
        slot, _ = iotas(128, 64)
        by_col = slots_of_strip(spec, 128, 64) & ~pulled(slot // 8, spec[0], 16)
        pick[...] = jnp.concatenate([one_hot(by_col), one_hot(by_row)], axis=1)

    slot, _ = iotas(128, PAIR)
    taken = pulled(slot % 8, spec[1], WIN) | pulled(slot // 8, spec[0], 16)
    for part, lanes in each_part():
        back = jnp.concatenate([strip[:, part, :, lanes].reshape(64, PAIR), row_strip_of(rows, part, lanes)], axis=0)
        moved = matmul(pick[...], back, 1, 0)
        put_tile(dqkv, att, part, lanes, jnp.where(taken, moved, tile_of(own_qkv, own_att, part, lanes)))


def window_kernel(
    spec, qkv, cot, hcol, hrow, table, gains, labels, att, dqkv, strip, sums, mask, table_grad, gain_grad, pick, send_pick
):
    step = pl.program_id(0)
    steps = pl.num_programs(0)
    shift_row, shift_col, grid_row, grid_col = spec[0], spec[1], spec[2], spec[3]
    tokens = 128
    col_place = lambda col: (col - shift_col) & 7
    score_scale = 1.0 / math.sqrt(HD)

    @pl.when(step == 0)
    def _():
        cols = labels.shape[0]
        rows = labels.shape[1]
        col_turn = jnp.where(shift_col <= HALF, WIN, cols - WIN)
        row_turn = jnp.where(shift_row <= HALF, 16, rows - 16)
        lane = lax.broadcasted_iota(jnp.int32, (8, 128), 1)
        sub = lax.broadcasted_iota(jnp.int32, (8, 128), 0)

        def labels_at(first_row):
            base = pl.multiple_of((first_row // 128) * 128, 128)
            here = labels[pl.ds(pl.multiple_of(grid_col, 8), 8), pl.ds(base, 128)]
            there = labels[pl.ds(pl.multiple_of((grid_col + col_turn) % cols, 8), 8), pl.ds(base, 128)]
            both = jnp.where(pulled(sub, shift_col, WIN), there, here).astype(jnp.float32)
            return pltpu.roll(both, (128 - first_row % 128) % 128, 1)

        slots = jnp.where(
            pulled(lane, shift_row, 16), labels_at((grid_row + row_turn) % rows), labels_at(grid_row)
        )
        across = jnp.concatenate([jnp.broadcast_to(slots[:, i : i + 1], (8, 128)) for i in range(16)], axis=0)
        query = lax.broadcasted_iota(jnp.int32, (tokens, tokens), 0) // 8
        key = lax.broadcasted_iota(jnp.int32, (tokens, tokens), 1) // 8
        same = (((query - shift_row) & 15) // 8) == (((key - shift_row) & 15) // 8)
        mask[...] = jnp.where(same & (across == across.T), 0.0, NEG_FILL)
        gain_grad[...] = jnp.zeros_like(gain_grad)
        slot, place = iotas(tokens, 32)
        row, col = row_slot(spec, place)
        slot_row, slot_col = split(slot, 8)
        by_row = (slot_row == row) & (slot_col == col) & pulled(row, shift_row, 16)
        by_row = one_hot(by_row & ~pulled(slot_col, shift_col, WIN))
        pick[...] = jnp.concatenate([one_hot(slots_of_strip(spec, tokens, 64)), by_row], axis=1)
        send_pick[...] = one_hot(strip_of_slots(spec, 64, tokens))

    slot, _ = iotas(tokens, PAIR)
    taken = pulled(slot % 8, shift_col, WIN) | pulled(slot // 8, shift_row, 16)

    pairs = range(WINDOW_HEADS * HD // PAIR)

    def load(part):
        both = []
        for pair in pairs:
            lanes = slice(pair * PAIR, pair * PAIR + PAIR)
            moved = jnp.concatenate(
                [hcol[:, part, :, lanes].reshape(64, PAIR), row_strip_of(hrow, part, lanes)], axis=0
            )
            tile = jnp.where(taken, matmul(pick[...], moved, 1, 0), tile_of(qkv, cot, part, lanes))
            both += [tile[:, :HD], tile[:, HD:]]
        return both

    def put(part, results):
        for pair in pairs:
            lanes = slice(pair * PAIR, pair * PAIR + PAIR)
            result = jnp.concatenate([results[2 * pair], results[2 * pair + 1]], axis=1)
            put_tile(dqkv, att, part, lanes, result)
            put_strip(strip, part, lanes, matmul(send_pick[...], result.astype(jnp.bfloat16), 1, 0))

    sub = lax.broadcasted_iota(jnp.int32, (8, 128), 0)
    lane = lax.broadcasted_iota(jnp.int32, (8, 128), 1)
    col_code = col_place(sub) - col_place(lane & 7) + WIN - 1
    gain_q = gains[0:1, :]
    gain_k = gains[1:2, :]

    heads = range(WINDOW_HEADS)

    queries = [head_norm(tile, gain_q) for tile in load(0)]
    keys = [head_norm(tile, gain_k) for tile in load(1)]
    values = [tile.astype(jnp.bfloat16) for tile in load(2)]
    grads = [tile.astype(jnp.bfloat16) for tile in load(3)]

    def bias(head):
        diagonal = jnp.zeros((8, 128), jnp.float32)
        for y in range(15):
            diagonal = jnp.where(col_code == y, table[head, y : y + 1, :], diagonal)
        return jnp.concatenate([pltpu.roll(diagonal, (row * 8 - 56) % 128, 1) for row in range(16)], axis=0)

    scores = [
        matmul(queries[head][2], keys[head][2], 1, 1) * score_scale + bias(head) + mask[...] for head in heads
    ]
    d_probs = [matmul(grads[head], values[head], 1, 1) for head in heads]
    tops = [jnp.max(scores[head], axis=-1, keepdims=True) for head in heads]
    weights = [jnp.exp(scores[head] - tops[head]) for head in heads]
    inverses = [1.0 / jnp.sum(weights[head], axis=-1, keepdims=True) for head in heads]
    row_dots = [jnp.sum(weights[head] * d_probs[head], axis=-1, keepdims=True) for head in heads]
    probs = [weights[head] * inverses[head] for head in heads]
    d_scores = [probs[head] * (d_probs[head] - row_dots[head] * inverses[head]) for head in heads]
    probs_b = [probs[head].astype(jnp.bfloat16) for head in heads]
    d_scores_b = [d_scores[head].astype(jnp.bfloat16) for head in heads]
    put(3, [matmul(probs_b[head], values[head], 1, 0) for head in heads])
    put(2, [matmul(probs_b[head], grads[head], 0, 0) for head in heads])
    d_qnorms = [matmul(d_scores_b[head], keys[head][2], 1, 0) for head in heads]
    d_knorms = [matmul(d_scores_b[head], queries[head][2], 0, 0) for head in heads]
    for head in heads:
        folded = functools.reduce(
            jnp.add,
            [pltpu.roll(d_scores[head][row * 8 : row * 8 + 8], (56 - row * 8) % 128, 1) for row in range(16)],
        )
        by_code = [jnp.sum(jnp.where(col_code == y, folded, 0.0), axis=0, keepdims=True) for y in range(15)]
        table_grad[pl.ds(pl.multiple_of((step * WINDOW_HEADS + head) * 16, 16), 16), :] = jnp.concatenate(
            by_code + [jnp.zeros((1, 128), jnp.float32)], axis=0
        )
    gain_grad[0] += functools.reduce(jnp.add, [fold_rows(d_qnorms[head] * queries[head][0]) for head in heads])
    gain_grad[1] += functools.reduce(jnp.add, [fold_rows(d_knorms[head] * keys[head][0]) for head in heads])
    put(0, [norm_back(*queries[head][:2], d_qnorms[head] * (gain_q * score_scale)) for head in heads])
    put(1, [norm_back(*keys[head][:2], d_knorms[head] * (gain_k * score_scale)) for head in heads])

    @pl.when(step == steps - 1)
    def _():
        group = lax.broadcasted_iota(jnp.int32, (16, 128), 0)
        member = lax.broadcasted_iota(jnp.int32, (16, 128), 1) // 8
        pick = jnp.where((group == member) & (group < 15), 1.0, 0.0)
        by_offset = matmul(pick, table_grad[...], 1, 1, precision=lax.Precision.HIGHEST)
        gain_q_sum = jnp.sum(gain_grad[0], axis=0, keepdims=True) * score_scale
        gain_k_sum = jnp.sum(gain_grad[1], axis=0, keepdims=True) * score_scale
        last = jnp.concatenate([gain_q_sum, gain_k_sum, jnp.zeros_like(gain_k_sum)], axis=1)
        is_last = lax.broadcasted_iota(jnp.int32, by_offset.shape, 0) == 15
        sums[...] = jnp.where(is_last, last, by_offset)


def qkv_spec(heads):
    return pl.BlockSpec((16, 3, 8, heads * HD), lambda i, s: (0, 0, 0, i))


def cot_spec(heads):
    return pl.BlockSpec((16, 8, heads * HD), lambda i, s: (0, 0, i))


def strip_spec(heads):
    return pl.BlockSpec((HALF, 4, 16, heads * HD), lambda i, s: (0, 0, 0, i))


def rows_spec(heads):
    return pl.BlockSpec((HALF, 4, 8, heads * HD), lambda i, s: (0, 0, 0, i))


def PICK(rows, cols):
    return pltpu.VMEM((rows, cols), jnp.bfloat16)


def bf16(*dims):
    return jax.ShapeDtypeStruct(dims, jnp.bfloat16)


def call(kernel, grid, in_specs, out_specs, out_shape, scratch, name, **kwargs):
    return pl.pallas_call(
        kernel,
        grid_spec=pltpu.PrefetchScalarGridSpec(
            num_scalar_prefetch=1, grid=grid, in_specs=in_specs, out_specs=out_specs, scratch_shapes=scratch
        ),
        out_shape=out_shape,
        compiler_params=pltpu.CompilerParams(dimension_semantics=("arbitrary",) * len(grid)),
        name=name,
        **kwargs,
    )


def pack_cols(spec, qkv, cot, hrow):
    width = cot.shape[2]
    n = MOVE_HEADS
    return call(
        pack_kernel,
        (width // (n * HD),),
        [qkv_spec(n), cot_spec(n), rows_spec(n)],
        strip_spec(n),
        bf16(HALF, 4, 16, width),
        [PICK(64, 128), PICK(64, 32)],
        "pack",
    )(spec, qkv, cot, hrow)


def pack_rows(spec, dqkv, att, strip):
    width = att.shape[2]
    n = MOVE_HEADS
    block = lambda s: jnp.where(s[0] <= HALF, 0, 3)
    return call(
        rows_kernel,
        (width // (n * HD),),
        [
            pl.BlockSpec((HALF, 3, 8, n * HD), lambda i, s: (block(s), 0, 0, i)),
            pl.BlockSpec((HALF, 8, n * HD), lambda i, s: (block(s), 0, i)),
            strip_spec(n),
        ],
        rows_spec(n),
        bf16(HALF, 4, 8, width),
        [PICK(32, 64)],
        "rows",
        cost_estimate=pl.CostEstimate(flops=10**9, transcendentals=0, bytes_accessed=3 * 10**6),
    )(spec, dqkv, att, strip)


def merge(spec, dqkv, att, strip, rows):
    width = att.shape[2]
    n = MOVE_HEADS
    return call(
        merge_kernel,
        (width // (n * HD),),
        [qkv_spec(n), cot_spec(n), strip_spec(n), rows_spec(n)],
        [qkv_spec(n), cot_spec(n)],
        [bf16(*dqkv.shape), bf16(*att.shape)],
        [PICK(128, 96)],
        "merge",
        cost_estimate=pl.CostEstimate(flops=2 * 10**9, transcendentals=0, bytes_accessed=9 * 10**6),
    )(spec, dqkv, att, strip, rows)


def run_windows(spec, qkv, cot, hcol, hrow, table, gains, labels):
    head_count = table.shape[0]
    n = WINDOW_HEADS
    return call(
        window_kernel,
        (head_count // n,),
        [
            qkv_spec(n),
            cot_spec(n),
            strip_spec(n),
            rows_spec(n),
            pl.BlockSpec((n, 16, 128), lambda i, s: (i, 0, 0)),
            pl.BlockSpec((2, 128), lambda i, s: (0, 0)),
            pl.BlockSpec(labels.shape, lambda i, s: (0, 0)),
        ],
        [cot_spec(n), qkv_spec(n), strip_spec(n), pl.BlockSpec((16, head_count * 16), lambda i, s: (0, 0))],
        [
            bf16(*cot.shape),
            bf16(*qkv.shape),
            bf16(*hcol.shape),
            jax.ShapeDtypeStruct((16, head_count * 16), jnp.float32),
        ],
        [
            pltpu.VMEM((128, 128), jnp.float32),
            pltpu.VMEM((head_count * 16, 128), jnp.float32),
            pltpu.VMEM((2, 8, 128), jnp.float32),
            PICK(128, 96),
            PICK(64, 128),
        ],
        "windows",
    )(spec, qkv, cot, hcol, hrow, table, gains, labels)


def spread(received, low):
    first = low % HALF
    spare = (first, HALF - first - received.shape[0], 0)
    return lax.pad(received, jnp.zeros((), received.dtype), (spare,) + ((0, 0, 0),) * (received.ndim - 1))


def case_of(shifts, axis):
    which, step = iotas(2, 3)
    return jnp.sum(((shifts[:, None] > 2 + step + (step > 0)) & (which == axis)).astype(jnp.int32))


def by_case(case, branch):
    return lax.switch(case, [branch(0, 2, -1), branch(0, 4, -1), branch(1, 4, 1), branch(2, 4, 1)])


def pull_rows(case, pieces, beside):
    def branch(first, last, steps):
        turn = 0 if steps < 0 else 12
        return lambda: (spread(shifted(pieces(first + turn, last + turn), ROW, steps), first), beside())

    return by_case(case, branch)


def pull_cols(index, packed):
    def branch(s):
        first, last, steps = (0, s, -1) if s <= HALF else (s - HALF, HALF, 1)
        return lambda: spread(shifted(packed[first:last], COL, steps), first)

    return lax.switch(index, [branch(s) for s in range(1, WIN)])


def doubled(sums, rounds):
    for axis, bit in rounds:
        sums = sums + lax.ppermute(sums, axis, [(i, i ^ bit) for i in range(lax.axis_size(axis))])
    return sums


def give_back(case, axis, strip, sums, rounds):
    def branch(first, last, steps):
        return lambda: (spread(shifted(strip[first:last], axis, -steps), first), doubled(sums, rounds))

    return by_case(case, branch)


def local(qkv, cotangent, norm_gains, rel_table, shifts, mask_ids):
    head_count = rel_table.shape[0]
    qkv_t = jnp.transpose(qkv, (0, 2, 1, 3))

    def row_pieces(low, high):
        return jnp.concatenate([qkv_t[low:high], cotangent[low:high, None]], axis=1)

    def tables():
        places = [lax.axis_index(ROW) * 16, lax.axis_index(COL) * 8]
        by_col = jnp.transpose(jnp.flip(rel_table, 1), (0, 2, 1))
        spread_out = jnp.pad(jnp.repeat(by_col, 8, axis=2), ((0, 0), (0, 1), (0, 8)))
        spec = jnp.stack([shifts[0], shifts[1]] + places).astype(jnp.int32)
        return spec, spread_out, case_of(shifts, 1), jnp.sum(shifts[1:]) - 1

    row_case = case_of(shifts, 0)
    hrow, (spec, table, col_case, col_index) = pull_rows(row_case, row_pieces, tables)
    packed = pack_cols(spec, qkv_t, cotangent, hrow)
    hcol = pull_cols(col_index, packed)
    att, dqkv, strip, sums = run_windows(spec, qkv_t, cotangent, hcol, hrow, table, norm_gains, mask_ids.T)
    strip, sums = give_back(col_case, COL, strip, sums, (("row_0", 1), ("row_0", 2), ("row_0", 4)))
    rows = pack_rows(spec, dqkv, att, strip)
    sums = doubled(sums, (("row_2", 1),))
    rows, sums = give_back(row_case, ROW, rows, sums, (("col_0", 1), ("col_0", 2)))
    dqkv, att = merge(spec, dqkv, att, strip, rows)
    sums = doubled(sums, (("col_1", 1), ("row_1", 1)))
    d_gains = sums[15, : 2 * HD].reshape(2, HD)
    d_table = jnp.transpose(jnp.flip(sums[:15], 0).reshape(15, head_count, 16)[:, :, :15], (1, 0, 2))
    return (att, jnp.transpose(dqkv, (0, 2, 1, 3)), d_gains, d_table)


def solution(mesh):
    torus = Mesh(mesh.devices.reshape(8, 2, 2, 4, 2), ROW_COL)
    placed = (P(ROW, COL, None, None), P(ROW, COL, None), P(), P(), P(), P())
    return jax.shard_map(
        local,
        mesh=torus,
        in_specs=placed,
        out_specs=(P(ROW, COL, None), P(ROW, COL, None, None), P(), P()),
        check_vma=False,
    )
```

```python
import functools
import math

import jax
import jax.numpy as jnp
from jax import lax
from jax.experimental import pallas as pl
from jax.experimental.pallas import tpu as pltpu
from jax.sharding import Mesh
from jax.sharding import PartitionSpec as P

ROW = ("row_0", "row_1", "row_2")
COL = ("col_0", "col_1")
ROW_COL = ("row_0", "row_1", "row_2", "col_0", "col_1")

EPSILON = 1e-06
NEG_FILL = -1e30
WIN = 8
HALF = 4
HD = 128
WINDOW_HEADS = 6
MOVE_HEADS = 12
PAIR = 256


def shifted(value, axis, steps):
    count = lax.axis_size(axis)
    pairs = [(source, (source + steps) % count) for source in range(count)]
    return lax.ppermute(value, axis, pairs)


def pulled(slot, shift, extent):
    low = jnp.where(shift <= HALF, 0, shift + extent - WIN)
    return (slot >= low) & (slot < jnp.where(shift <= HALF, shift, extent))


def head_norm(values, gain_vec):
    centred = values - jnp.mean(values, axis=-1, keepdims=True)
    variance = jnp.mean(centred * centred, axis=-1, keepdims=True)
    inv_sigma = lax.rsqrt(variance + EPSILON)
    x_hat = centred * inv_sigma
    return x_hat, inv_sigma, (x_hat * gain_vec).astype(jnp.bfloat16)


def norm_back(x_hat, inv_sigma, d_hat):
    first_mean = jnp.mean(d_hat, axis=-1, keepdims=True)
    second_mean = jnp.mean(d_hat * x_hat, axis=-1, keepdims=True)
    return inv_sigma * (d_hat - first_mean - x_hat * second_mean)


def fold_rows(values):
    return functools.reduce(jnp.add, [values[i * 8 : i * 8 + 8] for i in range(values.shape[0] // 8)])


def matmul(left, right, left_dim, right_dim, **kwargs):
    return lax.dot_general(
        left, right, (((left_dim,), (right_dim,)), ((), ())), preferred_element_type=jnp.float32, **kwargs
    )


def split(index, size):
    return index // size, index % size


def iotas(rows, cols):
    return (lax.broadcasted_iota(jnp.int32, (rows, cols), 0), lax.broadcasted_iota(jnp.int32, (rows, cols), 1))


def one_hot(condition):
    return jnp.where(condition, 1.0, 0.0).astype(jnp.bfloat16)


def strip_of_slots(spec, rows, cols):
    place, slot = iotas(rows, cols)
    (col, row), (slot_row, slot_col) = split(place, 16), split(slot, 8)
    return (row == slot_row) & (col + jnp.where(spec[1] <= HALF, 0, HALF) == slot_col)


def slots_of_strip(spec, rows, cols):
    slot, place = iotas(rows, cols)
    (col, row), (slot_row, slot_col) = split(place, 16), split(slot, 8)
    taken = (row == slot_row) & (col + jnp.where(spec[1] <= HALF, 0, HALF) == slot_col)
    return taken & pulled(slot_col, spec[1], WIN)


def row_slot(spec, place):
    row, col = split(place, 8)
    return row + jnp.where(spec[0] <= HALF, 0, 12), col


def tile_of(own_qkv, own_att, part, lanes):
    own = own_qkv[:, part, :, lanes] if part < 3 else own_att[:, :, lanes]
    return own.astype(jnp.float32).reshape(128, PAIR)


def row_strip_of(rows, part, lanes):
    return rows[:, part, :, lanes].astype(jnp.float32).reshape(32, PAIR).astype(jnp.bfloat16)


def put_tile(dqkv, att, part, lanes, result):
    rows = result.reshape(16, 8, PAIR).astype(jnp.bfloat16)
    if part < 3:
        dqkv[:, part, :, lanes] = rows
    else:
        att[:, :, lanes] = rows


def put_strip(strip, part, lanes, result):
    strip[:, part, :, lanes] = result.astype(jnp.bfloat16).reshape(HALF, 16, PAIR)


def each_part():
    return [(part, slice(at, at + PAIR)) for at in range(0, MOVE_HEADS * HD, PAIR) for part in range(4)]


def pack_kernel(spec, qkv, cot, hrow, strip, own_pick, row_pick):
    @pl.when(pl.program_id(0) == 0)
    def _():
        _, slot = iotas(64, 128)
        own_pick[...] = one_hot(strip_of_slots(spec, 64, 128) & ~pulled(slot // 8, spec[0], 16))
        place, source = iotas(64, 32)
        row, col = row_slot(spec, source)
        place_col, place_row = split(place, 16)
        same = (place_row == row) & (place_col + jnp.where(spec[1] <= HALF, 0, HALF) == col)
        row_pick[...] = one_hot(same & pulled(row, spec[0], 16))

    for part, lanes in each_part():
        own = tile_of(qkv, cot, part, lanes).astype(jnp.bfloat16)
        rows = row_strip_of(hrow, part, lanes)
        put_strip(strip, part, lanes, matmul(own_pick[...], own, 1, 0) + matmul(row_pick[...], rows, 1, 0))


def rows_kernel(spec, own_qkv, own_att, strip, rows, pick):
    @pl.when(pl.program_id(0) == 0)
    def _():
        slot, place = iotas(32, 64)
        row, slot_col = row_slot(spec, slot)
        col, place_row = split(place, 16)
        pick[...] = one_hot((row == place_row) & (col + jnp.where(spec[1] <= HALF, 0, HALF) == slot_col))

    slot, _ = iotas(32, PAIR)
    taken = pulled(slot % 8, spec[1], WIN)
    for part, lanes in each_part():
        own = own_qkv[:, part, :, lanes] if part < 3 else own_att[:, :, lanes]
        moved = matmul(pick[...], strip[:, part, :, lanes].reshape(64, PAIR), 1, 0)
        merged = jnp.where(taken, moved, own.astype(jnp.float32).reshape(32, PAIR))
        rows[:, part, :, lanes] = merged.reshape(HALF, 8, PAIR).astype(jnp.bfloat16)


def merge_kernel(spec, own_qkv, own_att, strip, rows, dqkv, att, pick):
    @pl.when(pl.program_id(0) == 0)
    def _():
        slot, place = iotas(128, 32)
        row, col = row_slot(spec, place)
        slot_row, slot_col = split(slot, 8)
        by_row = (slot_row == row) & (slot_col == col) & pulled(row, spec[0], 16)
        slot, _ = iotas(128, 64)
        by_col = slots_of_strip(spec, 128, 64) & ~pulled(slot // 8, spec[0], 16)
        pick[...] = jnp.concatenate([one_hot(by_col), one_hot(by_row)], axis=1)

    slot, _ = iotas(128, PAIR)
    taken = pulled(slot % 8, spec[1], WIN) | pulled(slot // 8, spec[0], 16)
    for part, lanes in each_part():
        back = jnp.concatenate([strip[:, part, :, lanes].reshape(64, PAIR), row_strip_of(rows, part, lanes)], axis=0)
        moved = matmul(pick[...], back, 1, 0)
        put_tile(dqkv, att, part, lanes, jnp.where(taken, moved, tile_of(own_qkv, own_att, part, lanes)))


def window_kernel(
    spec, qkv, cot, hcol, hrow, table, gains, labels, att, dqkv, strip, sums, mask, table_grad, gain_grad, pick, send_pick
):
    step = pl.program_id(0)
    steps = pl.num_programs(0)
    shift_row, shift_col, grid_row, grid_col = spec[0], spec[1], spec[2], spec[3]
    tokens = 128
    col_place = lambda col: (col - shift_col) & 7
    score_scale = 1.0 / math.sqrt(HD)

    @pl.when(step == 0)
    def _():
        cols = labels.shape[0]
        rows = labels.shape[1]
        col_turn = jnp.where(shift_col <= HALF, WIN, cols - WIN)
        row_turn = jnp.where(shift_row <= HALF, 16, rows - 16)
        lane = lax.broadcasted_iota(jnp.int32, (8, 128), 1)
        sub = lax.broadcasted_iota(jnp.int32, (8, 128), 0)

        def labels_at(first_row):
            base = pl.multiple_of((first_row // 128) * 128, 128)
            here = labels[pl.ds(pl.multiple_of(grid_col, 8), 8), pl.ds(base, 128)]
            there = labels[pl.ds(pl.multiple_of((grid_col + col_turn) % cols, 8), 8), pl.ds(base, 128)]
            both = jnp.where(pulled(sub, shift_col, WIN), there, here).astype(jnp.float32)
            return pltpu.roll(both, (128 - first_row % 128) % 128, 1)

        slots = jnp.where(
            pulled(lane, shift_row, 16), labels_at((grid_row + row_turn) % rows), labels_at(grid_row)
        )
        across = jnp.concatenate([jnp.broadcast_to(slots[:, i : i + 1], (8, 128)) for i in range(16)], axis=0)
        query = lax.broadcasted_iota(jnp.int32, (tokens, tokens), 0) // 8
        key = lax.broadcasted_iota(jnp.int32, (tokens, tokens), 1) // 8
        same = (((query - shift_row) & 15) // 8) == (((key - shift_row) & 15) // 8)
        mask[...] = jnp.where(same & (across == across.T), 0.0, NEG_FILL)
        gain_grad[...] = jnp.zeros_like(gain_grad)
        slot, place = iotas(tokens, 32)
        row, col = row_slot(spec, place)
        slot_row, slot_col = split(slot, 8)
        by_row = (slot_row == row) & (slot_col == col) & pulled(row, shift_row, 16)
        by_row = one_hot(by_row & ~pulled(slot_col, shift_col, WIN))
        pick[...] = jnp.concatenate([one_hot(slots_of_strip(spec, tokens, 64)), by_row], axis=1)
        send_pick[...] = one_hot(strip_of_slots(spec, 64, tokens))

    slot, _ = iotas(tokens, PAIR)
    taken = pulled(slot % 8, shift_col, WIN) | pulled(slot // 8, shift_row, 16)

    pairs = range(WINDOW_HEADS * HD // PAIR)

    def load(part):
        both = []
        for pair in pairs:
            lanes = slice(pair * PAIR, pair * PAIR + PAIR)
            moved = jnp.concatenate(
                [hcol[:, part, :, lanes].reshape(64, PAIR), row_strip_of(hrow, part, lanes)], axis=0
            )
            tile = jnp.where(taken, matmul(pick[...], moved, 1, 0), tile_of(qkv, cot, part, lanes))
            both += [tile[:, :HD], tile[:, HD:]]
        return both

    def put(part, results):
        for pair in pairs:
            lanes = slice(pair * PAIR, pair * PAIR + PAIR)
            result = jnp.concatenate([results[2 * pair], results[2 * pair + 1]], axis=1)
            put_tile(dqkv, att, part, lanes, result)
            put_strip(strip, part, lanes, matmul(send_pick[...], result.astype(jnp.bfloat16), 1, 0))

    sub = lax.broadcasted_iota(jnp.int32, (8, 128), 0)
    lane = lax.broadcasted_iota(jnp.int32, (8, 128), 1)
    col_code = col_place(sub) - col_place(lane & 7) + WIN - 1
    gain_q = gains[0:1, :]
    gain_k = gains[1:2, :]

    heads = range(WINDOW_HEADS)

    queries = [head_norm(tile, gain_q) for tile in load(0)]
    keys = [head_norm(tile, gain_k) for tile in load(1)]
    values = [tile.astype(jnp.bfloat16) for tile in load(2)]
    grads = [tile.astype(jnp.bfloat16) for tile in load(3)]

    def bias(head):
        diagonal = jnp.zeros((8, 128), jnp.float32)
        for y in range(15):
            diagonal = jnp.where(col_code == y, table[head, y : y + 1, :], diagonal)
        return jnp.concatenate([pltpu.roll(diagonal, (row * 8 - 56) % 128, 1) for row in range(16)], axis=0)

    scores = [
        matmul(queries[head][2], keys[head][2], 1, 1) * score_scale + bias(head) + mask[...] for head in heads
    ]
    d_probs = [matmul(grads[head], values[head], 1, 1) for head in heads]
    tops = [jnp.max(scores[head], axis=-1, keepdims=True) for head in heads]
    weights = [jnp.exp(scores[head] - tops[head]) for head in heads]
    inverses = [1.0 / jnp.sum(weights[head], axis=-1, keepdims=True) for head in heads]
    row_dots = [jnp.sum(weights[head] * d_probs[head], axis=-1, keepdims=True) for head in heads]
    probs = [weights[head] * inverses[head] for head in heads]
    d_scores = [probs[head] * (d_probs[head] - row_dots[head] * inverses[head]) for head in heads]
    probs_b = [probs[head].astype(jnp.bfloat16) for head in heads]
    d_scores_b = [d_scores[head].astype(jnp.bfloat16) for head in heads]
    put(3, [matmul(probs_b[head], values[head], 1, 0) for head in heads])
    put(2, [matmul(probs_b[head], grads[head], 0, 0) for head in heads])
    d_qnorms = [matmul(d_scores_b[head], keys[head][2], 1, 0) for head in heads]
    d_knorms = [matmul(d_scores_b[head], queries[head][2], 0, 0) for head in heads]
    for head in heads:
        folded = functools.reduce(
            jnp.add,
            [pltpu.roll(d_scores[head][row * 8 : row * 8 + 8], (56 - row * 8) % 128, 1) for row in range(16)],
        )
        by_code = [jnp.sum(jnp.where(col_code == y, folded, 0.0), axis=0, keepdims=True) for y in range(15)]
        table_grad[pl.ds(pl.multiple_of((step * WINDOW_HEADS + head) * 16, 16), 16), :] = jnp.concatenate(
            by_code + [jnp.zeros((1, 128), jnp.float32)], axis=0
        )
    gain_grad[0] += functools.reduce(jnp.add, [fold_rows(d_qnorms[head] * queries[head][0]) for head in heads])
    gain_grad[1] += functools.reduce(jnp.add, [fold_rows(d_knorms[head] * keys[head][0]) for head in heads])
    put(0, [norm_back(*queries[head][:2], d_qnorms[head] * (gain_q * score_scale)) for head in heads])
    put(1, [norm_back(*keys[head][:2], d_knorms[head] * (gain_k * score_scale)) for head in heads])

    @pl.when(step == steps - 1)
    def _():
        group = lax.broadcasted_iota(jnp.int32, (16, 128), 0)
        member = lax.broadcasted_iota(jnp.int32, (16, 128), 1) // 8
        pick = jnp.where((group == member) & (group < 15), 1.0, 0.0)
        by_offset = matmul(pick, table_grad[...], 1, 1, precision=lax.Precision.HIGHEST)
        gain_q_sum = jnp.sum(gain_grad[0], axis=0, keepdims=True) * score_scale
        gain_k_sum = jnp.sum(gain_grad[1], axis=0, keepdims=True) * score_scale
        last = jnp.concatenate([gain_q_sum, gain_k_sum, jnp.zeros_like(gain_k_sum)], axis=1)
        is_last = lax.broadcasted_iota(jnp.int32, by_offset.shape, 0) == 15
        sums[...] = jnp.where(is_last, last, by_offset)


def qkv_spec(heads):
    return pl.BlockSpec((16, 3, 8, heads * HD), lambda i, s: (0, 0, 0, i))


def cot_spec(heads):
    return pl.BlockSpec((16, 8, heads * HD), lambda i, s: (0, 0, i))


def strip_spec(heads):
    return pl.BlockSpec((HALF, 4, 16, heads * HD), lambda i, s: (0, 0, 0, i))


def rows_spec(heads):
    return pl.BlockSpec((HALF, 4, 8, heads * HD), lambda i, s: (0, 0, 0, i))


def PICK(rows, cols):
    return pltpu.VMEM((rows, cols), jnp.bfloat16)


def bf16(*dims):
    return jax.ShapeDtypeStruct(dims, jnp.bfloat16)


def call(kernel, grid, in_specs, out_specs, out_shape, scratch, name, **kwargs):
    return pl.pallas_call(
        kernel,
        grid_spec=pltpu.PrefetchScalarGridSpec(
            num_scalar_prefetch=1, grid=grid, in_specs=in_specs, out_specs=out_specs, scratch_shapes=scratch
        ),
        out_shape=out_shape,
        compiler_params=pltpu.CompilerParams(dimension_semantics=("arbitrary",) * len(grid)),
        name=name,
        **kwargs,
    )


def pack_cols(spec, qkv, cot, hrow):
    width = cot.shape[2]
    n = MOVE_HEADS
    return call(
        pack_kernel,
        (width // (n * HD),),
        [qkv_spec(n), cot_spec(n), rows_spec(n)],
        strip_spec(n),
        bf16(HALF, 4, 16, width),
        [PICK(64, 128), PICK(64, 32)],
        "pack",
    )(spec, qkv, cot, hrow)


def pack_rows(spec, dqkv, att, strip):
    width = att.shape[2]
    n = MOVE_HEADS
    block = lambda s: jnp.where(s[0] <= HALF, 0, 3)
    return call(
        rows_kernel,
        (width // (n * HD),),
        [
            pl.BlockSpec((HALF, 3, 8, n * HD), lambda i, s: (block(s), 0, 0, i)),
            pl.BlockSpec((HALF, 8, n * HD), lambda i, s: (block(s), 0, i)),
            strip_spec(n),
        ],
        rows_spec(n),
        bf16(HALF, 4, 8, width),
        [PICK(32, 64)],
        "rows",
        cost_estimate=pl.CostEstimate(flops=10**9, transcendentals=0, bytes_accessed=3 * 10**6),
    )(spec, dqkv, att, strip)


def merge(spec, dqkv, att, strip, rows):
    width = att.shape[2]
    n = MOVE_HEADS
    return call(
        merge_kernel,
        (width // (n * HD),),
        [qkv_spec(n), cot_spec(n), strip_spec(n), rows_spec(n)],
        [qkv_spec(n), cot_spec(n)],
        [bf16(*dqkv.shape), bf16(*att.shape)],
        [PICK(128, 96)],
        "merge",
        cost_estimate=pl.CostEstimate(flops=2 * 10**9, transcendentals=0, bytes_accessed=9 * 10**6),
    )(spec, dqkv, att, strip, rows)


def run_windows(spec, qkv, cot, hcol, hrow, table, gains, labels):
    head_count = table.shape[0]
    n = WINDOW_HEADS
    return call(
        window_kernel,
        (head_count // n,),
        [
            qkv_spec(n),
            cot_spec(n),
            strip_spec(n),
            rows_spec(n),
            pl.BlockSpec((n, 16, 128), lambda i, s: (i, 0, 0)),
            pl.BlockSpec((2, 128), lambda i, s: (0, 0)),
            pl.BlockSpec(labels.shape, lambda i, s: (0, 0)),
        ],
        [cot_spec(n), qkv_spec(n), strip_spec(n), pl.BlockSpec((16, head_count * 16), lambda i, s: (0, 0))],
        [
            bf16(*cot.shape),
            bf16(*qkv.shape),
            bf16(*hcol.shape),
            jax.ShapeDtypeStruct((16, head_count * 16), jnp.float32),
        ],
        [
            pltpu.VMEM((128, 128), jnp.float32),
            pltpu.VMEM((head_count * 16, 128), jnp.float32),
            pltpu.VMEM((2, 8, 128), jnp.float32),
            PICK(128, 96),
            PICK(64, 128),
        ],
        "windows",
    )(spec, qkv, cot, hcol, hrow, table, gains, labels)


def spread(received, low):
    first = low % HALF
    spare = (first, HALF - first - received.shape[0], 0)
    return lax.pad(received, jnp.zeros((), received.dtype), (spare,) + ((0, 0, 0),) * (received.ndim - 1))


def case_of(shifts, axis):
    which, step = iotas(2, 3)
    return jnp.sum(((shifts[:, None] > 2 + step + (step > 0)) & (which == axis)).astype(jnp.int32))


def by_case(case, branch):
    return lax.switch(case, [branch(0, 2, -1), branch(0, 4, -1), branch(1, 4, 1), branch(2, 4, 1)])


def pull_rows(case, pieces, beside):
    def branch(first, last, steps):
        turn = 0 if steps < 0 else 12
        return lambda: (spread(shifted(pieces(first + turn, last + turn), ROW, steps), first), beside())

    return by_case(case, branch)


def pull_cols(index, packed):
    def branch(s):
        first, last, steps = (0, s, -1) if s <= HALF else (s - HALF, HALF, 1)
        return lambda: spread(shifted(packed[first:last], COL, steps), first)

    return lax.switch(index, [branch(s) for s in range(1, WIN)])


def doubled(sums, rounds):
    for axis, bit in rounds:
        sums = sums + lax.ppermute(sums, axis, [(i, i ^ bit) for i in range(lax.axis_size(axis))])
    return sums


def give_back(case, axis, strip, sums, rounds):
    def branch(first, last, steps):
        return lambda: (spread(shifted(strip[first:last], axis, -steps), first), doubled(sums, rounds))

    return by_case(case, branch)


def local(qkv, cotangent, norm_gains, rel_table, shifts, mask_ids):
    head_count = rel_table.shape[0]
    qkv_t = jnp.transpose(qkv, (0, 2, 1, 3))

    def row_pieces(low, high):
        return jnp.concatenate([qkv_t[low:high], cotangent[low:high, None]], axis=1)

    def tables():
        places = [lax.axis_index(ROW) * 16, lax.axis_index(COL) * 8]
        by_col = jnp.transpose(jnp.flip(rel_table, 1), (0, 2, 1))
        spread_out = jnp.pad(jnp.repeat(by_col, 8, axis=2), ((0, 0), (0, 1), (0, 8)))
        spec = jnp.stack([shifts[0], shifts[1]] + places).astype(jnp.int32)
        return spec, spread_out, case_of(shifts, 1), jnp.sum(shifts[1:]) - 1

    row_case = case_of(shifts, 0)
    hrow, (spec, table, col_case, col_index) = pull_rows(row_case, row_pieces, tables)
    packed = pack_cols(spec, qkv_t, cotangent, hrow)
    hcol = pull_cols(col_index, packed)
    att, dqkv, strip, sums = run_windows(spec, qkv_t, cotangent, hcol, hrow, table, norm_gains, mask_ids.T)
    strip, sums = give_back(col_case, COL, strip, sums, (("row_0", 1), ("row_0", 2), ("row_0", 4)))
    rows = pack_rows(spec, dqkv, att, strip)
    sums = doubled(sums, (("col_1", 1),))
    rows, sums = give_back(row_case, ROW, rows, sums, (("col_0", 1), ("col_0", 2)))
    dqkv, att = merge(spec, dqkv, att, strip, rows)
    sums = doubled(sums, (("row_2", 1), ("row_1", 1)))
    d_gains = sums[15, : 2 * HD].reshape(2, HD)
    d_table = jnp.transpose(jnp.flip(sums[:15], 0).reshape(15, head_count, 16)[:, :, :15], (1, 0, 2))
    return (att, jnp.transpose(dqkv, (0, 2, 1, 3)), d_gains, d_table)


def solution(mesh):
    torus = Mesh(mesh.devices.reshape(8, 2, 2, 4, 2), ROW_COL)
    placed = (P(ROW, COL, None, None), P(ROW, COL, None), P(), P(), P(), P())
    return jax.shard_map(
        local,
        mesh=torus,
        in_specs=placed,
        out_specs=(P(ROW, COL, None), P(ROW, COL, None, None), P(), P()),
        check_vma=False,
    )
```

```python
import functools
import math

import jax
import jax.numpy as jnp
from jax import lax
from jax.experimental import pallas as pl
from jax.experimental.pallas import tpu as pltpu
from jax.sharding import Mesh
from jax.sharding import PartitionSpec as P

ROW = ("row_0", "row_1", "row_2")
COL = ("col_0", "col_1")
ROW_COL = ("row_0", "row_1", "row_2", "col_0", "col_1")

EPSILON = 1e-06
NEG_FILL = -1e30
WIN = 8
HALF = 4
HD = 128
WINDOW_HEADS = 6
MOVE_HEADS = 8
PAIR = 256


def shifted(value, axis, steps):
    count = lax.axis_size(axis)
    pairs = [(source, (source + steps) % count) for source in range(count)]
    return lax.ppermute(value, axis, pairs)


def pulled(slot, shift, extent):
    low = jnp.where(shift <= HALF, 0, shift + extent - WIN)
    return (slot >= low) & (slot < jnp.where(shift <= HALF, shift, extent))


def head_norm(values, gain_vec):
    centred = values - jnp.mean(values, axis=-1, keepdims=True)
    variance = jnp.mean(centred * centred, axis=-1, keepdims=True)
    inv_sigma = lax.rsqrt(variance + EPSILON)
    x_hat = centred * inv_sigma
    return x_hat, inv_sigma, (x_hat * gain_vec).astype(jnp.bfloat16)


def norm_back(x_hat, inv_sigma, d_hat):
    first_mean = jnp.mean(d_hat, axis=-1, keepdims=True)
    second_mean = jnp.mean(d_hat * x_hat, axis=-1, keepdims=True)
    return inv_sigma * (d_hat - first_mean - x_hat * second_mean)


def fold_rows(values):
    return functools.reduce(jnp.add, [values[i * 8 : i * 8 + 8] for i in range(values.shape[0] // 8)])


def matmul(left, right, left_dim, right_dim, **kwargs):
    return lax.dot_general(
        left, right, (((left_dim,), (right_dim,)), ((), ())), preferred_element_type=jnp.float32, **kwargs
    )


def split(index, size):
    return index // size, index % size


def iotas(rows, cols):
    return (lax.broadcasted_iota(jnp.int32, (rows, cols), 0), lax.broadcasted_iota(jnp.int32, (rows, cols), 1))


def one_hot(condition):
    return jnp.where(condition, 1.0, 0.0).astype(jnp.bfloat16)


def strip_of_slots(spec, rows, cols):
    place, slot = iotas(rows, cols)
    (col, row), (slot_row, slot_col) = split(place, 16), split(slot, 8)
    return (row == slot_row) & (col + jnp.where(spec[1] <= HALF, 0, HALF) == slot_col)


def slots_of_strip(spec, rows, cols):
    slot, place = iotas(rows, cols)
    (col, row), (slot_row, slot_col) = split(place, 16), split(slot, 8)
    taken = (row == slot_row) & (col + jnp.where(spec[1] <= HALF, 0, HALF) == slot_col)
    return taken & pulled(slot_col, spec[1], WIN)


def row_slot(spec, place):
    row, col = split(place, 8)
    return row + jnp.where(spec[0] <= HALF, 0, 12), col


def tile_of(own_qkv, own_att, part, lanes):
    own = own_qkv[:, part, :, lanes] if part < 3 else own_att[:, :, lanes]
    return own.astype(jnp.float32).reshape(128, PAIR)


def row_strip_of(rows, part, lanes):
    return rows[:, part, :, lanes].astype(jnp.float32).reshape(32, PAIR).astype(jnp.bfloat16)


def put_tile(dqkv, att, part, lanes, result):
    rows = result.reshape(16, 8, PAIR).astype(jnp.bfloat16)
    if part < 3:
        dqkv[:, part, :, lanes] = rows
    else:
        att[:, :, lanes] = rows


def put_strip(strip, part, lanes, result):
    strip[:, part, :, lanes] = result.astype(jnp.bfloat16).reshape(HALF, 16, PAIR)


def each_part():
    return [(part, slice(at, at + PAIR)) for at in range(0, MOVE_HEADS * HD, PAIR) for part in range(4)]


def pack_kernel(spec, qkv, cot, hrow, strip, own_pick, row_pick):
    @pl.when(pl.program_id(0) == 0)
    def _():
        _, slot = iotas(64, 128)
        own_pick[...] = one_hot(strip_of_slots(spec, 64, 128) & ~pulled(slot // 8, spec[0], 16))
        place, source = iotas(64, 32)
        row, col = row_slot(spec, source)
        place_col, place_row = split(place, 16)
        same = (place_row == row) & (place_col + jnp.where(spec[1] <= HALF, 0, HALF) == col)
        row_pick[...] = one_hot(same & pulled(row, spec[0], 16))

    for part, lanes in each_part():
        own = tile_of(qkv, cot, part, lanes).astype(jnp.bfloat16)
        rows = row_strip_of(hrow, part, lanes)
        put_strip(strip, part, lanes, matmul(own_pick[...], own, 1, 0) + matmul(row_pick[...], rows, 1, 0))


def rows_kernel(spec, own_qkv, own_att, strip, rows, pick):
    @pl.when(pl.program_id(0) == 0)
    def _():
        slot, place = iotas(32, 64)
        row, slot_col = row_slot(spec, slot)
        col, place_row = split(place, 16)
        pick[...] = one_hot((row == place_row) & (col + jnp.where(spec[1] <= HALF, 0, HALF) == slot_col))

    slot, _ = iotas(32, PAIR)
    taken = pulled(slot % 8, spec[1], WIN)
    for part, lanes in each_part():
        own = own_qkv[:, part, :, lanes] if part < 3 else own_att[:, :, lanes]
        moved = matmul(pick[...], strip[:, part, :, lanes].reshape(64, PAIR), 1, 0)
        merged = jnp.where(taken, moved, own.astype(jnp.float32).reshape(32, PAIR))
        rows[:, part, :, lanes] = merged.reshape(HALF, 8, PAIR).astype(jnp.bfloat16)


def merge_kernel(spec, own_qkv, own_att, strip, rows, dqkv, att, pick):
    @pl.when(pl.program_id(0) == 0)
    def _():
        slot, place = iotas(128, 32)
        row, col = row_slot(spec, place)
        slot_row, slot_col = split(slot, 8)
        by_row = (slot_row == row) & (slot_col == col) & pulled(row, spec[0], 16)
        slot, _ = iotas(128, 64)
        by_col = slots_of_strip(spec, 128, 64) & ~pulled(slot // 8, spec[0], 16)
        pick[...] = jnp.concatenate([one_hot(by_col), one_hot(by_row)], axis=1)

    slot, _ = iotas(128, PAIR)
    taken = pulled(slot % 8, spec[1], WIN) | pulled(slot // 8, spec[0], 16)
    for part, lanes in each_part():
        back = jnp.concatenate([strip[:, part, :, lanes].reshape(64, PAIR), row_strip_of(rows, part, lanes)], axis=0)
        moved = matmul(pick[...], back, 1, 0)
        put_tile(dqkv, att, part, lanes, jnp.where(taken, moved, tile_of(own_qkv, own_att, part, lanes)))


def window_kernel(
    spec, qkv, cot, hcol, hrow, table, gains, labels, att, dqkv, strip, sums, mask, table_grad, gain_grad, pick, send_pick
):
    step = pl.program_id(0)
    steps = pl.num_programs(0)
    shift_row, shift_col, grid_row, grid_col = spec[0], spec[1], spec[2], spec[3]
    tokens = 128
    col_place = lambda col: (col - shift_col) & 7
    score_scale = 1.0 / math.sqrt(HD)

    @pl.when(step == 0)
    def _():
        cols = labels.shape[0]
        rows = labels.shape[1]
        col_turn = jnp.where(shift_col <= HALF, WIN, cols - WIN)
        row_turn = jnp.where(shift_row <= HALF, 16, rows - 16)
        lane = lax.broadcasted_iota(jnp.int32, (8, 128), 1)
        sub = lax.broadcasted_iota(jnp.int32, (8, 128), 0)

        def labels_at(first_row):
            base = pl.multiple_of((first_row // 128) * 128, 128)
            here = labels[pl.ds(pl.multiple_of(grid_col, 8), 8), pl.ds(base, 128)]
            there = labels[pl.ds(pl.multiple_of((grid_col + col_turn) % cols, 8), 8), pl.ds(base, 128)]
            both = jnp.where(pulled(sub, shift_col, WIN), there, here).astype(jnp.float32)
            return pltpu.roll(both, (128 - first_row % 128) % 128, 1)

        slots = jnp.where(
            pulled(lane, shift_row, 16), labels_at((grid_row + row_turn) % rows), labels_at(grid_row)
        )
        across = jnp.concatenate([jnp.broadcast_to(slots[:, i : i + 1], (8, 128)) for i in range(16)], axis=0)
        query = lax.broadcasted_iota(jnp.int32, (tokens, tokens), 0) // 8
        key = lax.broadcasted_iota(jnp.int32, (tokens, tokens), 1) // 8
        same = (((query - shift_row) & 15) // 8) == (((key - shift_row) & 15) // 8)
        mask[...] = jnp.where(same & (across == across.T), 0.0, NEG_FILL)
        gain_grad[...] = jnp.zeros_like(gain_grad)
        slot, place = iotas(tokens, 32)
        row, col = row_slot(spec, place)
        slot_row, slot_col = split(slot, 8)
        by_row = (slot_row == row) & (slot_col == col) & pulled(row, shift_row, 16)
        by_row = one_hot(by_row & ~pulled(slot_col, shift_col, WIN))
        pick[...] = jnp.concatenate([one_hot(slots_of_strip(spec, tokens, 64)), by_row], axis=1)
        send_pick[...] = one_hot(strip_of_slots(spec, 64, tokens))

    slot, _ = iotas(tokens, PAIR)
    taken = pulled(slot % 8, shift_col, WIN) | pulled(slot // 8, shift_row, 16)

    pairs = range(WINDOW_HEADS * HD // PAIR)

    def load(part):
        both = []
        for pair in pairs:
            lanes = slice(pair * PAIR, pair * PAIR + PAIR)
            moved = jnp.concatenate(
                [hcol[:, part, :, lanes].reshape(64, PAIR), row_strip_of(hrow, part, lanes)], axis=0
            )
            tile = jnp.where(taken, matmul(pick[...], moved, 1, 0), tile_of(qkv, cot, part, lanes))
            both += [tile[:, :HD], tile[:, HD:]]
        return both

    def put(part, results):
        for pair in pairs:
            lanes = slice(pair * PAIR, pair * PAIR + PAIR)
            result = jnp.concatenate([results[2 * pair], results[2 * pair + 1]], axis=1)
            put_tile(dqkv, att, part, lanes, result)
            put_strip(strip, part, lanes, matmul(send_pick[...], result.astype(jnp.bfloat16), 1, 0))

    sub = lax.broadcasted_iota(jnp.int32, (8, 128), 0)
    lane = lax.broadcasted_iota(jnp.int32, (8, 128), 1)
    col_code = col_place(sub) - col_place(lane & 7) + WIN - 1
    gain_q = gains[0:1, :]
    gain_k = gains[1:2, :]

    heads = range(WINDOW_HEADS)

    queries = [head_norm(tile, gain_q) for tile in load(0)]
    keys = [head_norm(tile, gain_k) for tile in load(1)]
    values = [tile.astype(jnp.bfloat16) for tile in load(2)]
    grads = [tile.astype(jnp.bfloat16) for tile in load(3)]

    def bias(head):
        diagonal = jnp.zeros((8, 128), jnp.float32)
        for y in range(15):
            diagonal = jnp.where(col_code == y, table[head, y : y + 1, :], diagonal)
        return jnp.concatenate([pltpu.roll(diagonal, (row * 8 - 56) % 128, 1) for row in range(16)], axis=0)

    scores = [
        matmul(queries[head][2], keys[head][2], 1, 1) * score_scale + bias(head) + mask[...] for head in heads
    ]
    d_probs = [matmul(grads[head], values[head], 1, 1) for head in heads]
    tops = [jnp.max(scores[head], axis=-1, keepdims=True) for head in heads]
    weights = [jnp.exp(scores[head] - tops[head]) for head in heads]
    inverses = [1.0 / jnp.sum(weights[head], axis=-1, keepdims=True) for head in heads]
    row_dots = [jnp.sum(weights[head] * d_probs[head], axis=-1, keepdims=True) for head in heads]
    probs = [weights[head] * inverses[head] for head in heads]
    d_scores = [probs[head] * (d_probs[head] - row_dots[head] * inverses[head]) for head in heads]
    probs_b = [probs[head].astype(jnp.bfloat16) for head in heads]
    d_scores_b = [d_scores[head].astype(jnp.bfloat16) for head in heads]
    put(3, [matmul(probs_b[head], values[head], 1, 0) for head in heads])
    put(2, [matmul(probs_b[head], grads[head], 0, 0) for head in heads])
    d_qnorms = [matmul(d_scores_b[head], keys[head][2], 1, 0) for head in heads]
    d_knorms = [matmul(d_scores_b[head], queries[head][2], 0, 0) for head in heads]
    for head in heads:
        folded = functools.reduce(
            jnp.add,
            [pltpu.roll(d_scores[head][row * 8 : row * 8 + 8], (56 - row * 8) % 128, 1) for row in range(16)],
        )
        by_code = [jnp.sum(jnp.where(col_code == y, folded, 0.0), axis=0, keepdims=True) for y in range(15)]
        table_grad[pl.ds(pl.multiple_of((step * WINDOW_HEADS + head) * 16, 16), 16), :] = jnp.concatenate(
            by_code + [jnp.zeros((1, 128), jnp.float32)], axis=0
        )
    gain_grad[0] += functools.reduce(jnp.add, [fold_rows(d_qnorms[head] * queries[head][0]) for head in heads])
    gain_grad[1] += functools.reduce(jnp.add, [fold_rows(d_knorms[head] * keys[head][0]) for head in heads])
    put(0, [norm_back(*queries[head][:2], d_qnorms[head] * (gain_q * score_scale)) for head in heads])
    put(1, [norm_back(*keys[head][:2], d_knorms[head] * (gain_k * score_scale)) for head in heads])

    @pl.when(step == steps - 1)
    def _():
        group = lax.broadcasted_iota(jnp.int32, (16, 128), 0)
        member = lax.broadcasted_iota(jnp.int32, (16, 128), 1) // 8
        pick = jnp.where((group == member) & (group < 15), 1.0, 0.0)
        by_offset = matmul(pick, table_grad[...], 1, 1, precision=lax.Precision.HIGHEST)
        gain_q_sum = jnp.sum(gain_grad[0], axis=0, keepdims=True) * score_scale
        gain_k_sum = jnp.sum(gain_grad[1], axis=0, keepdims=True) * score_scale
        last = jnp.concatenate([gain_q_sum, gain_k_sum, jnp.zeros_like(gain_k_sum)], axis=1)
        is_last = lax.broadcasted_iota(jnp.int32, by_offset.shape, 0) == 15
        sums[...] = jnp.where(is_last, last, by_offset)


def qkv_spec(heads):
    return pl.BlockSpec((16, 3, 8, heads * HD), lambda i, s: (0, 0, 0, i))


def cot_spec(heads):
    return pl.BlockSpec((16, 8, heads * HD), lambda i, s: (0, 0, i))


def strip_spec(heads):
    return pl.BlockSpec((HALF, 4, 16, heads * HD), lambda i, s: (0, 0, 0, i))


def rows_spec(heads):
    return pl.BlockSpec((HALF, 4, 8, heads * HD), lambda i, s: (0, 0, 0, i))


def PICK(rows, cols):
    return pltpu.VMEM((rows, cols), jnp.bfloat16)


def bf16(*dims):
    return jax.ShapeDtypeStruct(dims, jnp.bfloat16)


def call(kernel, grid, in_specs, out_specs, out_shape, scratch, name, **kwargs):
    return pl.pallas_call(
        kernel,
        grid_spec=pltpu.PrefetchScalarGridSpec(
            num_scalar_prefetch=1, grid=grid, in_specs=in_specs, out_specs=out_specs, scratch_shapes=scratch
        ),
        out_shape=out_shape,
        compiler_params=pltpu.CompilerParams(dimension_semantics=("arbitrary",) * len(grid)),
        name=name,
        **kwargs,
    )


def pack_cols(spec, qkv, cot, hrow):
    width = cot.shape[2]
    n = MOVE_HEADS
    return call(
        pack_kernel,
        (width // (n * HD),),
        [qkv_spec(n), cot_spec(n), rows_spec(n)],
        strip_spec(n),
        bf16(HALF, 4, 16, width),
        [PICK(64, 128), PICK(64, 32)],
        "pack",
    )(spec, qkv, cot, hrow)


def pack_rows(spec, dqkv, att, strip):
    width = att.shape[2]
    n = MOVE_HEADS
    block = lambda s: jnp.where(s[0] <= HALF, 0, 3)
    return call(
        rows_kernel,
        (width // (n * HD),),
        [
            pl.BlockSpec((HALF, 3, 8, n * HD), lambda i, s: (block(s), 0, 0, i)),
            pl.BlockSpec((HALF, 8, n * HD), lambda i, s: (block(s), 0, i)),
            strip_spec(n),
        ],
        rows_spec(n),
        bf16(HALF, 4, 8, width),
        [PICK(32, 64)],
        "rows",
        cost_estimate=pl.CostEstimate(flops=10**9, transcendentals=0, bytes_accessed=3 * 10**6),
    )(spec, dqkv, att, strip)


def merge(spec, dqkv, att, strip, rows):
    width = att.shape[2]
    n = MOVE_HEADS
    return call(
        merge_kernel,
        (width // (n * HD),),
        [qkv_spec(n), cot_spec(n), strip_spec(n), rows_spec(n)],
        [qkv_spec(n), cot_spec(n)],
        [bf16(*dqkv.shape), bf16(*att.shape)],
        [PICK(128, 96)],
        "merge",
        cost_estimate=pl.CostEstimate(flops=2 * 10**9, transcendentals=0, bytes_accessed=9 * 10**6),
    )(spec, dqkv, att, strip, rows)


def run_windows(spec, qkv, cot, hcol, hrow, table, gains, labels):
    head_count = table.shape[0]
    n = WINDOW_HEADS
    return call(
        window_kernel,
        (head_count // n,),
        [
            qkv_spec(n),
            cot_spec(n),
            strip_spec(n),
            rows_spec(n),
            pl.BlockSpec((n, 16, 128), lambda i, s: (i, 0, 0)),
            pl.BlockSpec((2, 128), lambda i, s: (0, 0)),
            pl.BlockSpec(labels.shape, lambda i, s: (0, 0)),
        ],
        [cot_spec(n), qkv_spec(n), strip_spec(n), pl.BlockSpec((16, head_count * 16), lambda i, s: (0, 0))],
        [
            bf16(*cot.shape),
            bf16(*qkv.shape),
            bf16(*hcol.shape),
            jax.ShapeDtypeStruct((16, head_count * 16), jnp.float32),
        ],
        [
            pltpu.VMEM((128, 128), jnp.float32),
            pltpu.VMEM((head_count * 16, 128), jnp.float32),
            pltpu.VMEM((2, 8, 128), jnp.float32),
            PICK(128, 96),
            PICK(64, 128),
        ],
        "windows",
    )(spec, qkv, cot, hcol, hrow, table, gains, labels)


def spread(received, low):
    first = low % HALF
    spare = (first, HALF - first - received.shape[0], 0)
    return lax.pad(received, jnp.zeros((), received.dtype), (spare,) + ((0, 0, 0),) * (received.ndim - 1))


def case_of(shifts, axis):
    which, step = iotas(2, 3)
    return jnp.sum(((shifts[:, None] > 2 + step + (step > 0)) & (which == axis)).astype(jnp.int32))


def by_case(case, branch):
    return lax.switch(case, [branch(0, 2, -1), branch(0, 4, -1), branch(1, 4, 1), branch(2, 4, 1)])


def pull_rows(case, pieces, beside):
    def branch(first, last, steps):
        turn = 0 if steps < 0 else 12
        return lambda: (spread(shifted(pieces(first + turn, last + turn), ROW, steps), first), beside())

    return by_case(case, branch)


def pull_cols(index, packed):
    def branch(s):
        first, last, steps = (0, s, -1) if s <= HALF else (s - HALF, HALF, 1)
        return lambda: spread(shifted(packed[first:last], COL, steps), first)

    return lax.switch(index, [branch(s) for s in range(1, WIN)])


def doubled(sums, rounds):
    for axis, bit in rounds:
        sums = sums + lax.ppermute(sums, axis, [(i, i ^ bit) for i in range(lax.axis_size(axis))])
    return sums


def give_back(case, axis, strip, sums, rounds):
    def branch(first, last, steps):
        return lambda: (spread(shifted(strip[first:last], axis, -steps), first), doubled(sums, rounds))

    return by_case(case, branch)


def local(qkv, cotangent, norm_gains, rel_table, shifts, mask_ids):
    head_count = rel_table.shape[0]
    qkv_t = jnp.transpose(qkv, (0, 2, 1, 3))

    def row_pieces(low, high):
        return jnp.concatenate([qkv_t[low:high], cotangent[low:high, None]], axis=1)

    def tables():
        places = [lax.axis_index(ROW) * 16, lax.axis_index(COL) * 8]
        by_col = jnp.transpose(jnp.flip(rel_table, 1), (0, 2, 1))
        spread_out = jnp.pad(jnp.repeat(by_col, 8, axis=2), ((0, 0), (0, 1), (0, 8)))
        spec = jnp.stack([shifts[0], shifts[1]] + places).astype(jnp.int32)
        return spec, spread_out, case_of(shifts, 1), jnp.sum(shifts[1:]) - 1

    row_case = case_of(shifts, 0)
    hrow, (spec, table, col_case, col_index) = pull_rows(row_case, row_pieces, tables)
    packed = pack_cols(spec, qkv_t, cotangent, hrow)
    hcol = pull_cols(col_index, packed)
    att, dqkv, strip, sums = run_windows(spec, qkv_t, cotangent, hcol, hrow, table, norm_gains, mask_ids.T)
    strip, sums = give_back(col_case, COL, strip, sums, (("row_0", 1), ("row_0", 2), ("row_0", 4)))
    rows = pack_rows(spec, dqkv, att, strip)
    sums = doubled(sums, (("row_2", 1),))
    rows, sums = give_back(row_case, ROW, rows, sums, (("col_0", 1), ("col_0", 2)))
    dqkv, att = merge(spec, dqkv, att, strip, rows)
    sums = doubled(sums, (("col_1", 1), ("row_1", 1)))
    d_gains = sums[15, : 2 * HD].reshape(2, HD)
    d_table = jnp.transpose(jnp.flip(sums[:15], 0).reshape(15, head_count, 16)[:, :, :15], (1, 0, 2))
    return (att, jnp.transpose(dqkv, (0, 2, 1, 3)), d_gains, d_table)


def solution(mesh):
    torus = Mesh(mesh.devices.reshape(8, 2, 2, 4, 2), ROW_COL)
    placed = (P(ROW, COL, None, None), P(ROW, COL, None), P(), P(), P(), P())
    return jax.shard_map(
        local,
        mesh=torus,
        in_specs=placed,
        out_specs=(P(ROW, COL, None), P(ROW, COL, None, None), P(), P()),
        check_vma=False,
    )
```
